128 devices in a mesh: row: 16 (over z, x_lo, core), col: 8 (over y, x_hi).
Axes of the slice: x: 4 (x_hi: 2, x_lo: 2; x = x_hi * 2 + x_lo), y: 4, z: 4, core: 2. Of those that a mesh axis runs over, the one named last changes fastest.
Arguments:
- loadings: bfloat16 [8, 32768, 1024], P(None, 'row', 'col'), may hold values from -6 to 6
- weights: bfloat16 [8, 32768, 512], P(None, 'row', 'col'), may hold values from -0.03125 to 0.03125
- specific: float32 [8, 32768], P(None, 'row'), may hold values from 0.2 to 5
- factor_cov: float32 [8, 1024, 1024], P(None, 'col'), may hold values from -0.001953125 to 0.0048828125, as said below
Outputs:
- portfolio_cov: float32 [8, 512, 512], P(None, 'row', 'col')
The draws below stay inside these ranges and needn't reach their ends.
Inputs may be any that keep to these rules, and one draw needn't show every extreme that they name: `factor_cov`: each day's matrix is a symmetric positive definite factor covariance of order 1024.
All inputs are finite; a program needn't handle non-finite values.
Results may differ from the reference program's by a relative error of at most 0.0003.
Values may be sent and summed in bfloat16 or wider, within the bound.
A program may use at most 128 MiB of HBM per device.

```python
import math
import jax
import jax.numpy as jnp
from jax import lax

N = 32768
R = 1024
K = 512
DAYS = 8


def draw_factor_cov(key, part):
    first_key, second_key = jax.random.split(jax.random.fold_in(key, 11))
    noise = jax.random.normal(first_key, (DAYS, R, R), jnp.float32)
    symmetric = (noise + jnp.swapaxes(noise, 1, 2)) / jnp.sqrt(2.0 * R)
    variances = jax.random.uniform(second_key, (DAYS, R), jnp.float32, 1.0, 3.0)
    identity = jnp.eye(R, dtype=jnp.float32)
    return (identity[None, :, :] * variances[:, :, None] + 0.4 * symmetric) / R


def steps_of(rng, extent, pieces, smallest, largest):
    loudness, own = 1.0, jax.random.fold_in(rng, 6)
    for position, parts in pieces:
        steps = jnp.exp(jax.random.uniform(jax.random.fold_in(own, position), (parts,), jnp.float32, smallest / len(pieces), largest / len(pieces)))
        loudness = loudness * jnp.repeat(steps, extent[position] // parts).reshape([-1 if axis == position else 1 for axis in range(len(extent))])
    return loudness


def normal_values(rng, dims, spread, reach, cuts=(), kind=jnp.bfloat16):
    result = spread * jax.random.normal(rng, dims, jnp.float32)
    if cuts:
        result = result * steps_of(rng, dims, cuts, -0.22, 0.18)
    return jnp.clip(result, -reach, reach).astype(kind)


def setup_inputs(seed: int = 0) -> dict:
    keys = jax.random.split(jax.random.key(seed), 5)
    return {
        "loadings": normal_values(keys[0], (DAYS, N, R), 1.0, 6.0, ((1, 16), (2, 8))),
        "weights": normal_values(keys[1], (DAYS, N, K), N ** -0.5, 0.03125, ((1, 16), (2, 8))),
        "specific": jnp.clip(jnp.exp(math.log(5.0) - 3.218876 * jax.random.uniform(keys[2], (DAYS, N), jnp.float32) ** steps_of(keys[2], (DAYS, N), ((1, 16),), -0.2, 0.2)), 0.2, 5.0),
        "factor_cov": draw_factor_cov(jax.random.fold_in(keys[4], 71), 0),
    }


def one_day(operands):
    loadings, weights, specific, factor_cov = operands
    exposure = jnp.dot(loadings.T, weights, preferred_element_type=jnp.float32)
    weighted = (specific[:, None] * weights.astype(jnp.float32)).astype(jnp.bfloat16)
    specific_cov = jnp.dot(weights.T, weighted, preferred_element_type=jnp.float32)
    left = jnp.dot(exposure.T, factor_cov, precision=lax.Precision.HIGHEST)
    return jnp.dot(left, exposure, precision=lax.Precision.HIGHEST) + specific_cov


def reference(loadings, weights, specific, factor_cov):
    return lax.map(one_day, (loadings, weights, specific, factor_cov))
```

```python
import jax
import jax.numpy as jnp
from jax import lax
from jax.experimental import pallas as pl
from jax.experimental.pallas import tpu as pltpu
from jax.sharding import PartitionSpec as P

MESH = pl.DeviceIdType.MESH
F32 = jnp.float32
BF16 = jnp.bfloat16
NT = (((1,), (1,)), ((), ()))
SLOT = {0: 0, 2: 1, 1: 2, 3: 3}


def kernel(load_ref, wt_ref, spec_ref, fcov_ref, out_ref,
           wt_all, l_all, wg, f_rows,
           part_s, part_o, part_n, part_f,
           send_s, send_o, send_n, send_f,
           got_s, got_o, got_n, got_f,
           rs_s, rs_o, rs_n, rs_f,
           red, s_red, s_all, e_all, left_val, left_buf, obuf, oin,
           wy_s, wy_r, ly_s, ly_r, wx_s, wx_r, loc, f_s, f_r,
           cc_s, cc_r, rss_s, rss_r, ag_s, ag_r, sx_s, sx_r, la_s, la_r, fo_s, fo_r):
    row, col = lax.axis_index("row"), lax.axis_index("col")
    z, xl, core = row // 4, (row // 2) % 2, row % 2
    y, xh = col // 2, col % 2
    ports = 2 * z + xl

    def dev(z_, xl_, core_, y_, xh_):
        return (z_ * 4 + xl_ * 2 + core_, y_ * 2 + xh_)

    def remote(src, dst, ssem, rsem, to):
        return pltpu.make_async_remote_copy(
            src_ref=src, dst_ref=dst, send_sem=ssem, recv_sem=rsem,
            device_id=to, device_id_type=MESH)

    bar = pltpu.get_barrier_semaphore()

    def greet(k, _):
        a = (core * 8 + y * 2 + xh + k) % 16
        pl.semaphore_signal(bar, inc=1, device_id=dev(z, xl, a // 8, (a // 2) % 4, a % 2), device_id_type=MESH)
        b = (z * 4 + xl * 2 + xh + k) % 16
        pl.semaphore_signal(bar, inc=1, device_id=dev(b // 4, (b // 2) % 2, core, y, b % 2), device_id_type=MESH)
        return 0

    lax.fori_loop(1, 16, greet, 0)
    pl.semaphore_wait(bar, 30)

    def at64(i):
        return pl.ds(pl.multiple_of(i * 64, 64), 64)

    def at128(i):
        return pl.ds(pl.multiple_of(i * 128, 128), 128)

    own_w = []
    for dl in range(2):
        c = pltpu.make_async_copy(wt_ref.at[2 * y + dl], wt_all.at[dl, at64(col), :], loc.at[dl])
        c.start()
        own_w.append(c)
    wy = {}
    for dl in range(2):
        for dy in (1, 3, 2):
            ty = (y + dy) % 4
            c = remote(wt_ref.at[2 * ty + dl], wt_all.at[dl, at64(col), :],
                       wy_s.at[dy - 1, dl], wy_r.at[dy - 1, dl], dev(z, xl, core, ty, xh))
            c.start()
            wy[dy, dl] = c
    wx = {}
    for dl in range(2):
        c = remote(wt_ref.at[2 * y + dl], wt_all.at[dl, at64(col), :],
                   wx_s.at[0, dl], wx_r.at[0, dl], dev(z, xl, core, y, 1 - xh))
        c.start()
        wx[0, dl] = c
    own_l = []
    for dl in range(2):
        c = pltpu.make_async_copy(load_ref.at[2 * y + dl], l_all.at[dl, :, pl.ds(0, 128)], loc.at[2 + dl])
        c.start()
        own_l.append(c)
    ly = {}
    for dy in (1, 3, 2):
        for dl in range(2):
            ty = (y + dy) % 4
            rel = 4 - dy
            c = remote(load_ref.at[2 * ty + dl], l_all.at[dl, :, pl.ds(128 * SLOT[rel], 128)],
                       ly_s.at[dy - 1, dl], ly_r.at[dy - 1, dl], dev(z, xl, core, ty, xh))
            c.start()
            ly[dy, dl] = c
    turn = jnp.where(core == 0, z, 4 - z)
    yq = (y + turn) % 4
    yd = (y + 4 - turn) % 4
    f_copy = remote(fcov_ref.at[2 * yd + core], f_rows, f_s, f_r, dev(z, xl, core, yd, xh))
    f_own = pltpu.make_async_copy(fcov_ref.at[2 * y + core], f_rows, loc.at[4])

    @pl.when(z == 0)
    def _():
        f_own.start()

    @pl.when(z != 0)
    def _():
        f_copy.start()

    for dl in range(2):
        for rel in (1, 3, 2):
            sy = (y + rel) % 4
            wy[4 - rel, dl].wait_recv()
            rows = at64(2 * sy + xh)
            c = remote(wt_all.at[dl, rows, :], wt_all.at[dl, rows, :],
                       wx_s.at[rel, dl], wx_r.at[rel, dl], dev(z, xl, core, y, 1 - xh))
            c.start()
            wx[rel, dl] = c
    for c in own_w + own_l:
        c.wait()
    for dl in range(2):
        scale = spec_ref[pl.ds(2 * y + dl, 1), :]
        for b in range(4):
            w = wt_all[dl, at64(2 * b + xh), :]
            wg[dl, pl.ds(64 * b, 64), :] = (scale * w.astype(F32)).astype(BF16)
    for dl in range(2):
        for rel in (0, 1, 3, 2):
            wx[rel, dl].wait_recv()

    mate = dev(z, xl, 1 - core, y, xh)

    def both(part, send, got, i, product):
        send[...] = product(1 - core)
        c = remote(send, got, cc_s.at[i], cc_r.at[i], mate)
        c.start()
        part[...] = product(core)
        return c

    def spread(part, got, rs, i, pair):
        pair.wait_recv()
        part[...] = part[...] + got[...]

        def go(k, _):
            to = (ports + k) % 8
            remote(part.at[at64(to), :], rs.at[k - 1], rss_s.at[i, k - 1], rss_r.at[i, k - 1],
                   dev(to // 2, to % 2, core, y, xh)).start()
            return 0

        lax.fori_loop(1, 8, go, 0)

    def rs_wait(part, rs, i):
        def one(k, _):
            remote(part.at[at64(0), :], rs.at[k], rss_s.at[i, k], rss_r.at[i, k], mate).wait_recv()
            return 0

        lax.fori_loop(0, 7, one, 0)
        total = part[at64(ports), :]
        for k in range(7):
            total = total + rs[k]
        return total

    def gather(value, u, rel):
        block = 2 * ((y + rel) % 4) + xh
        red[u] = value
        e_all[at64(ports), at128(block)] = value

        def go(k, _):
            b = (z * 4 + xl * 2 + xh + k) % 16
            remote(red.at[u], e_all.at[at64(ports), at128(block)], ag_s.at[u, k - 1], ag_r.at[u, k - 1],
                   dev(b // 4, (b // 2) % 2, core, y, b % 2)).start()
            return 0

        lax.fori_loop(1, 16, go, 0)

    def l_dot(lo, n):
        def product(d):
            return jnp.dot(wt_all[d], l_all[d, :, pl.ds(lo, n)], preferred_element_type=F32)

        return product

    def s_dot(d):
        return lax.dot_general(wt_all[d], wg[d], NT, preferred_element_type=F32)

    pair_s = both(part_s, send_s, got_s, 0, s_dot)
    pair_o = both(part_o, send_o, got_o, 1, l_dot(0, 128))
    spread(part_s, got_s, rs_s, 0, pair_s)
    spread(part_o, got_o, rs_o, 1, pair_o)
    for dy in (1, 3):
        for dl in range(2):
            ly[dy, dl].wait_recv()
    pair_n = both(part_n, send_n, got_n, 2, l_dot(256, 256))
    spread(part_n, got_n, rs_n, 2, pair_n)
    s_red[...] = rs_wait(part_s, rs_s, 0)
    mine = pl.ds(pl.multiple_of(xh * 32, 32), 32)
    theirs = pl.ds(pl.multiple_of((1 - xh) * 32, 32), 32)
    s_copy = remote(s_red.at[theirs, :], s_all.at[xh], sx_s, sx_r, dev(z, xl, core, y, 1 - xh))
    s_copy.start()
    s_all[xh] = s_red[mine, :]
    gather(rs_wait(part_o, rs_o, 1), 0, 0)
    both_n = rs_wait(part_n, rs_n, 2)
    gather(both_n[:, :128], 1, 1)
    gather(both_n[:, 128:], 2, 3)
    for dl in range(2):
        ly[2, dl].wait_recv()
    pair_f = both(part_f, send_f, got_f, 3, l_dot(128, 128))
    spread(part_f, got_f, rs_f, 3, pair_f)
    gather(rs_wait(part_f, rs_f, 3), 3, 2)

    def ag_wait(i, _):
        u, k = i // 15, i % 15
        remote(red.at[u], e_all.at[at64(0), at128(0)], ag_s.at[u, k], ag_r.at[u, k], mate).wait_recv()
        return 0

    lax.fori_loop(0, 60, ag_wait, 0)

    @pl.when(z == 0)
    def _():
        f_own.wait()

    @pl.when(z != 0)
    def _():
        f_copy.wait_recv()

    e_rows = jnp.concatenate([e_all[at64(2 * b + xl), :] for b in range(4)], axis=0)
    left_val[...] = lax.dot_general(e_rows, f_rows[...], NT, precision=lax.Precision.HIGHEST,
                                    preferred_element_type=F32)
    block = 2 * yq + xh
    me8 = 2 * z + xh

    def rows32(i):
        return pl.ds(pl.multiple_of(i * 32, 32), 32)

    def la(k):
        to = (me8 + k) % 8
        return remote(left_val.at[rows32(to), :], left_buf.at[:, at128(block)], la_s.at[k - 1], la_r.at[k - 1],
                      dev(to // 2, xl, core, y, to % 2))

    def la_go(k, _):
        la(k).start()
        return 0

    lax.fori_loop(1, 8, la_go, 0)
    left_buf[:, at128(block)] = left_val[rows32(me8), :]

    def la_wait(k, _):
        la(k).wait_recv()
        return 0

    lax.fori_loop(1, 8, la_wait, 0)
    factor = lax.dot_general(left_buf[...], e_all[...], NT, precision=lax.Precision.HIGHEST,
                             preferred_element_type=F32)
    s_copy.wait_recv()
    for c in range(8):
        obuf[c] = factor[:, 64 * c:64 * c + 64] + s_all[c % 2, :, 64 * (c // 2):64 * (c // 2) + 64]
    day = 2 * y + core
    base = core * 8 + y * 2 + xh
    goal = xh * 8

    def fo(c):
        return remote(obuf.at[c], oin.at[day], fo_s.at[c], fo_r.at[day], dev(z, xl, xh, c // 2, c % 2))

    def fo_go(c, _):
        @pl.when(goal + c != base)
        def _():
            fo(c).start()

        return 0

    lax.fori_loop(0, 8, fo_go, 0)

    @pl.when(xh == core)
    def _():
        oin[day] = obuf[col]

    def fo_wait(d, _):
        @pl.when((d % 2) * 8 + (d // 2) * 2 + core != base)
        def _():
            remote(obuf.at[0], oin.at[d], fo_s.at[0], fo_r.at[d], mate).wait_recv()

        return 0

    lax.fori_loop(0, 8, fo_wait, 0)
    out_ref[...] = oin[...]

    for c in [*wy.values(), *wx.values(), *ly.values(), pair_s, pair_o, pair_n, pair_f, s_copy]:
        c.wait_send()

    @pl.when(z != 0)
    def _():
        f_copy.wait_send()

    for i, (part, rs) in enumerate(((part_s, rs_s), (part_o, rs_o), (part_n, rs_n), (part_f, rs_f))):
        def rs_sent(k, _, part=part, rs=rs, i=i):
            remote(part.at[at64(0), :], rs.at[k], rss_s.at[i, k], rss_r.at[i, k], mate).wait_send()
            return 0

        lax.fori_loop(0, 7, rs_sent, 0)

    def ag_sent(i, _):
        u, k = i // 15, i % 15
        remote(red.at[u], e_all.at[at64(0), at128(0)], ag_s.at[u, k], ag_r.at[u, k], mate).wait_send()
        return 0

    lax.fori_loop(0, 60, ag_sent, 0)

    def la_sent(k, _):
        la(k).wait_send()
        return 0

    lax.fori_loop(1, 8, la_sent, 0)

    def fo_sent(c, _):
        @pl.when(goal + c != base)
        def _():
            fo(c).wait_send()

        return 0

    lax.fori_loop(0, 8, fo_sent, 0)


def shards(loadings, weights, specific, factor_cov):
    assets = loadings.shape[1]
    wt = jnp.swapaxes(weights, 1, 2)
    any_ = pl.BlockSpec(memory_space=pl.ANY)
    vmem = pl.BlockSpec(memory_space=pltpu.VMEM)
    dma = pltpu.SemaphoreType.DMA
    widths = (256, 128, 256, 128)
    return pl.pallas_call(
        kernel,
        out_shape=jax.ShapeDtypeStruct((8, 32, 64), F32),
        in_specs=[any_, any_, vmem, any_],
        out_specs=vmem,
        scratch_shapes=[
            pltpu.VMEM((2, 512, assets), BF16),
            pltpu.VMEM((2, assets, 512), BF16),
            pltpu.VMEM((2, 256, assets), BF16),
            pltpu.VMEM((128, 1024), F32),
            *[pltpu.VMEM((512, w), F32) for w in widths],
            *[pltpu.VMEM((512, w), F32) for w in widths],
            *[pltpu.VMEM((512, w), F32) for w in widths],
            *[pltpu.VMEM((7, 64, w), F32) for w in widths],
            pltpu.VMEM((4, 64, 128), F32),
            pltpu.VMEM((64, 256), F32),
            pltpu.VMEM((2, 32, 256), F32),
            pltpu.VMEM((512, 1024), F32),
            pltpu.VMEM((256, 128), F32),
            pltpu.VMEM((32, 1024), F32),
            pltpu.VMEM((8, 32, 64), F32),
            pltpu.VMEM((8, 32, 64), F32),
            dma((3, 2)), dma((3, 2)), dma((3, 2)), dma((3, 2)), dma((4, 2)), dma((4, 2)), dma((5,)), dma, dma,
            dma((4,)), dma((4,)), dma((4, 7)), dma((4, 7)), dma((4, 15)), dma((4, 15)), dma, dma,
            dma((7,)), dma((7,)), dma((8,)), dma((8,)),
        ],
        compiler_params=pltpu.CompilerParams(collective_id=0, has_side_effects=True),
    )(loadings, wt, specific, factor_cov)


def solution(mesh):
    in_specs = (P(None, "row", "col"), P(None, "row", "col"), P(None, "row"), P(None, "col", None))
    out_specs = P(None, "row", "col")
    return jax.shard_map(shards, mesh=mesh, in_specs=in_specs, out_specs=out_specs, check_vma=False)
```

```python
import jax
import jax.numpy as jnp
from jax import lax
from jax.experimental import pallas as pl
from jax.experimental.pallas import tpu as pltpu
from jax.sharding import PartitionSpec as P

MESH = pl.DeviceIdType.MESH
F32 = jnp.float32
BF16 = jnp.bfloat16
HIGH = lax.Precision.HIGHEST
NT = (((1,), (1,)), ((), ()))
SLOT = {0: 0, 2: 1, 1: 2, 3: 3}


def kernel(load_ref, wt_ref, spec_ref, fcov_ref, out_ref,
           wt_all, l_all, w_pass, l_pass, wg, f_rows,
           part_o, part_f, part_s, send_o, send_f, send_s, got_o, got_f, got_s,
           xg_o, xg_f, xg_s, zg_o, zg_f, zg_s,
           two, got_n, rs_n, red, s_red, s_tile, e_all, left_val, left_buf, obuf, oin,
           wy_s, wy_r, ly_s, ly_r, wx_s, wx_r, wf_s, wf_r, lf_s, lf_r, loc, f_s, f_r,
           cc_s, cc_r, xl_s, xl_r, zz_s, zz_r, rn_s, rn_r, ag_s, ag_r, sx_s, sx_r,
           la_s, la_r, fo_s, fo_r):
    row, col = lax.axis_index("row"), lax.axis_index("col")
    z, xl, core = row // 4, (row // 2) % 2, row % 2
    y, xh = col // 2, col % 2
    day = 2 * y + core

    def dev(z_, xl_, core_, y_, xh_):
        return (z_ * 4 + xl_ * 2 + core_, y_ * 2 + xh_)

    def remote(src, dst, ssem, rsem, to):
        return pltpu.make_async_remote_copy(
            src_ref=src, dst_ref=dst, send_sem=ssem, recv_sem=rsem,
            device_id=to, device_id_type=MESH)

    def loop(lo, hi, body):
        def step(k, _):
            body(k)
            return 0

        lax.fori_loop(lo, hi, step, 0)

    def part64(i):
        return pl.ds(pl.multiple_of(i * 64, 64), 64)

    def lanes128(i):
        return pl.ds(pl.multiple_of(i * 128, 128), 128)

    def lanes256(i):
        return pl.ds(pl.multiple_of(i * 256, 256), 256)

    bar = pltpu.get_barrier_semaphore()

    def greet(to):
        pl.semaphore_signal(bar, inc=1, device_id=to, device_id_type=MESH)

    def greet_line(k):
        a = (core * 4 + y + k) % 8
        greet(dev(z, xl, a // 4, a % 4, xh))

    def greet_plane(k):
        b = (z * 4 + xl * 2 + xh + k) % 16
        greet(dev(b // 4, (b // 2) % 2, core, y, b % 2))

    def greet_swap(k):
        greet(dev(z, xh, k // 4, k % 4, xl))

    loop(1, 8, greet_line)
    loop(1, 16, greet_plane)

    @pl.when(xl != xh)
    def _():
        loop(0, 8, greet_swap)
        pl.semaphore_wait(bar, 30)

    @pl.when(xl == xh)
    def _():
        pl.semaphore_wait(bar, 22)

    def block_of(b):
        return part64(4 * xh + b)

    here = block_of(y)
    across = dev(z, xl, core, y, 1 - xh)
    near = (1, 3)
    own = []
    wy, wx, ly, wf, lf = {}, {}, {}, {}, {}

    def w_near(dy, dl):
        ty = (y + dy) % 4
        wy[dy, dl] = remote(wt_ref.at[2 * ty + dl], wt_all.at[dl, here, :],
                            wy_s.at[dy - 1, dl], wy_r.at[dy - 1, dl], dev(z, xl, core, ty, xh))
        wy[dy, dl].start()

    def w_across(rel, dl):
        rows = block_of((y + rel) % 4)
        src = wt_ref.at[2 * y + dl] if rel == 0 else wt_all.at[dl, rows, :]
        wx[rel, dl] = remote(src, wt_all.at[dl, rows, :], wx_s.at[rel, dl], wx_r.at[rel, dl], across)
        wx[rel, dl].start()

    def w_arrived(rel, dl):
        wy[4 - rel, dl].wait_recv()
        w_across(rel, dl)

    def l_near(dy, dl):
        ty = (y + dy) % 4
        ly[dy, dl] = remote(load_ref.at[2 * ty + dl], l_all.at[dl, :, pl.ds(128 * SLOT[4 - dy], 128)],
                            ly_s.at[dy - 1, dl], ly_r.at[dy - 1, dl], dev(z, xl, core, ty, xh))
        ly[dy, dl].start()

    for dy in near:
        w_near(dy, 0)
    for dl in range(2):
        w_across(0, dl)
        own.append(pltpu.make_async_copy(wt_ref.at[2 * y + dl], wt_all.at[dl, here, :], loc.at[dl]))
        own[-1].start()
    for dl in range(2):
        wf[dl] = remote(wt_ref.at[2 * ((y + 2) % 4) + dl], w_pass.at[dl], wf_s.at[dl], wf_r.at[dl],
                        dev(z, xl, core, (y + near[dl]) % 4, xh))
        wf[dl].start()
    for dy in near:
        w_near(dy, 1)
    for dl in range(2):
        own.append(pltpu.make_async_copy(load_ref.at[2 * y + dl], l_all.at[dl, :, pl.ds(0, 128)], loc.at[2 + dl]))
        own[-1].start()
    w_arrived(1, 0)
    w_arrived(3, 0)
    for dl in range(2):
        wf[dl].wait_recv()
        wy[2, dl] = remote(w_pass.at[dl], wt_all.at[dl, block_of((y + near[1 - dl]) % 4), :],
                           wy_s.at[1, dl], wy_r.at[1, dl], dev(z, xl, core, (y + near[dl]) % 4, xh))
        wy[2, dl].start()
    for dl in range(2):
        lf[dl] = remote(load_ref.at[2 * ((y + 2) % 4) + dl], l_pass.at[dl], lf_s.at[dl], lf_r.at[dl],
                        dev(z, xl, core, (y + near[dl]) % 4, xh))
        lf[dl].start()
    for dy in near:
        l_near(dy, 0)
    w_arrived(1, 1)
    w_arrived(3, 1)
    w_arrived(2, 0)
    w_arrived(2, 1)
    for c in own:
        c.wait()
    for dl in range(2):
        scale = spec_ref[pl.ds(2 * y + dl, 1), :]
        w = wt_all[dl, lanes256(xh), :]
        wg[dl] = (scale * w.astype(F32)).astype(BF16)
    for dl in range(2):
        lf[dl].wait_recv()
        ly[2, dl] = remote(l_pass.at[dl], l_all.at[dl, :, pl.ds(128 * SLOT[2], 128)],
                           ly_s.at[1, dl], ly_r.at[1, dl], dev(z, xl, core, (y + near[dl]) % 4, xh))
        ly[2, dl].start()
    for dy in near:
        l_near(dy, 1)
    turn = (z + 2 * core) % 4
    yq = (y + turn) % 4
    yd = (y + 4 - turn) % 4
    f_copy = remote(fcov_ref.at[2 * yd + core], f_rows, f_s, f_r, dev(z, xl, core, yd, xh))
    f_own = pltpu.make_async_copy(fcov_ref.at[day], f_rows, loc.at[4])

    @pl.when(turn == 0)
    def _():
        f_own.start()

    @pl.when(turn != 0)
    def _():
        f_copy.start()

    for dl in range(2):
        for rel in (0, 1, 3, 2):
            wx[rel, dl].wait_recv()
    mate = dev(z, xl, 1 - core, y, xh)
    beside = dev(z, 1 - xl, core, y, xh)
    kept, given = lanes256(xl), lanes256(1 - xl)

    def l_dot(lo, n):
        def product(d):
            return jnp.dot(wt_all[d], l_all[d, :, pl.ds(lo, n)], preferred_element_type=F32)

        return product

    def s_dot(d):
        return lax.dot_general(wt_all[d], wg[d], NT, preferred_element_type=F32)

    class Group:
        def __init__(self, i, part, send, got, xg, zg, product):
            self.i, self.part, self.send, self.got, self.xg, self.zg = i, part, send, got, xg, zg
            self.product = product
            self.pair = remote(send, got, cc_s.at[i], cc_r.at[i], mate)
            self.side = remote(part.at[given, :], xg, xl_s.at[i], xl_r.at[i], beside)

        def dots(self):
            self.send[...] = self.product(1 - core)
            self.pair.start()
            self.part[...] = self.product(core)

        def over_x(self):
            self.pair.wait_recv()
            self.part[given, :] = self.part[given, :] + self.got[given, :]
            self.side.start()
            self.part[kept, :] = self.part[kept, :] + self.got[kept, :]

        def line(self, k):
            to = (z + k) % 4
            return remote(self.xg.at[part64(to), :], self.zg.at[k - 1],
                          zz_s.at[self.i, k - 1], zz_r.at[self.i, k - 1], dev(to, xl, core, y, xh))

        def over_z(self):
            self.side.wait_recv()
            self.xg[...] = self.xg[...] + self.part[kept, :]
            for k in (1, 3, 2):
                self.line(k).start()

        def total(self):
            for k in (1, 3, 2):
                self.line(k).wait_recv()
            return (self.xg[part64(z), :] + self.zg[0]) + (self.zg[1] + self.zg[2])

        def sent(self):
            self.pair.wait_send()
            self.side.wait_send()
            for k in (1, 3, 2):
                self.line(k).wait_send()

    me8 = 2 * z + xh

    def spread(u, k, block):
        b = (me8 + k) % 8
        return remote(red.at[u], e_all.at[part64(z), lanes128(block)], ag_s.at[u, k - 1], ag_r.at[u, k - 1],
                      dev(b // 2, xl, core, y, b % 2))

    def gather(value, u, rel):
        block = 2 * ((y + rel) % 4) + xh
        red[u] = value
        loop(1, 8, lambda k: spread(u, k, block).start())
        e_all[part64(z), lanes128(block)] = value

    g_o = Group(0, part_o, send_o, got_o, xg_o, zg_o, l_dot(0, 128))
    g_f = Group(1, part_f, send_f, got_f, xg_f, zg_f, l_dot(128, 128))
    g_s = Group(2, part_s, send_s, got_s, xg_s, zg_s, s_dot)

    me_p = 4 * xl + z

    def pair_n(dl):
        return remote(two.at[dl], got_n, cc_s.at[3], cc_r.at[3], mate)

    def rn(k):
        p = (me_p + k) % 8
        return remote(two.at[core, part64(p), :], rs_n.at[k - 1], rn_s.at[k - 1], rn_r.at[k - 1],
                      dev(p % 4, p // 4, core, y, xh))

    def near_dot(dl):
        for dy in near:
            ly[dy, dl].wait_recv()
        two[dl] = jnp.dot(wt_all[dl], l_all[dl, :, pl.ds(256, 256)], preferred_element_type=F32)

        @pl.when(core != dl)
        def _():
            pair_n(dl).start()

    def near_add(dl):
        @pl.when(core == dl)
        def _():
            pair_n(dl).wait_recv()
            two[dl] = two[dl] + got_n[...]
            loop(1, 8, lambda k: rn(k).start())

    def near_gather(dl):
        @pl.when(core == dl)
        def _():
            loop(1, 8, lambda k: rn(k).wait_recv())
            total = two[dl, part64(me_p), :]
            for k in range(7):
                total = total + rs_n[k]
            gather(total[:, :128], 2, 1)
            gather(total[:, 128:], 3, 3)

    g_o.dots()
    g_o.over_x()
    near_dot(0)
    g_s.dots()
    g_o.over_z()
    near_add(0)
    g_s.over_x()
    gather(g_o.total(), 0, 0)
    for dl in range(2):
        ly[2, dl].wait_recv()
    g_f.dots()
    g_f.over_x()
    g_s.over_z()
    near_gather(0)
    g_f.over_z()
    swap = remote(s_red, s_tile, sx_s, sx_r, dev(z, xh, core, y, xl))
    s_red[...] = g_s.total()

    @pl.when(xl != xh)
    def _():
        swap.start()

    @pl.when(xl == xh)
    def _():
        s_tile[...] = s_red[...]

    for c in [*wy.values(), *wx.values(), *wf.values()]:
        c.wait_send()
    gather(g_f.total(), 1, 2)
    near_dot(1)
    near_add(1)

    @pl.when(turn == 0)
    def _():
        f_own.wait()

    @pl.when(turn != 0)
    def _():
        f_copy.wait_recv()

    def left_part(u, rel):
        loop(1, 8, lambda k: spread(u, k, 0).wait_recv())
        at = lanes256((y + rel) % 4)
        return lax.dot_general(e_all[:, at], f_rows[:, at], NT, precision=HIGH, preferred_element_type=F32)

    left_val[...] = left_part(0, 0) + left_part(1, 2)
    for g in (g_o, g_f, g_s):
        g.sent()
    near_gather(1)
    left_val[...] += left_part(2, 1) + left_part(3, 3)

    def la(j):
        return remote(left_val.at[part64(j // 2), :], left_buf.at[:, lanes128(2 * yq + xh)],
                      la_s.at[j], la_r.at[me8], dev(j // 2, j % 2, core, y, xl))

    alike = xl == xh
    me_t = 2 * z + xl

    def unless(skip, body):
        @pl.when(jnp.logical_not(skip))
        def _():
            body()

    loop(0, 8, lambda j: unless(jnp.logical_and(alike, j == me_t), lambda: la(j).start()))

    @pl.when(alike)
    def _():
        left_buf[:, lanes128(2 * yq + xh)] = left_val[part64(z), :]

    for u in range(4):
        loop(1, 8, lambda k, u=u: spread(u, k, 0).wait_send())
    loop(1, 8, lambda k: rn(k).wait_send())

    def la_in(j):
        return remote(left_val.at[part64(0), :], left_buf.at[:, lanes128(0)], la_s.at[0], la_r.at[j], mate)

    loop(0, 8, lambda j: unless(jnp.logical_and(alike, j == me8), lambda: la_in(j).wait_recv()))
    tile = lax.dot_general(left_buf[...], e_all[...], NT, precision=HIGH, preferred_element_type=F32)

    @pl.when(xl != xh)
    def _():
        swap.wait_recv()

    tile = tile + s_tile[...]
    for h in range(2):
        for b in range(4):
            obuf[4 * h + b] = tile[32 * h:32 * h + 32, 64 * b:64 * b + 64]

    def fo(i):
        return remote(obuf.at[i], oin.at[day], fo_s.at[i], fo_r.at[day], dev(z, xh, i // 4, i % 4, xl))

    me_o = 4 * core + y
    loop(0, 8, lambda i: unless(jnp.logical_and(alike, i == me_o), lambda: fo(i).start()))

    @pl.when(alike)
    def _():
        oin[day] = obuf[me_o]

    for c in [*ly.values(), *lf.values()]:
        c.wait_send()
    pair_n(1 - core).wait_send()

    @pl.when(xl != xh)
    def _():
        swap.wait_send()

    @pl.when(turn != 0)
    def _():
        f_copy.wait_send()

    loop(0, 8, lambda j: unless(jnp.logical_and(alike, j == me_t), lambda: la(j).wait_send()))

    def fo_in(d):
        return remote(obuf.at[0], oin.at[d], fo_s.at[0], fo_r.at[d], mate)

    loop(0, 8, lambda d: unless(jnp.logical_and(alike, d == day), lambda: fo_in(d).wait_recv()))
    out_ref[...] = oin[...]
    loop(0, 8, lambda i: unless(jnp.logical_and(alike, i == me_o), lambda: fo(i).wait_send()))


def shards(loadings, weights, specific, factor_cov):
    assets = loadings.shape[1]
    wt = jnp.swapaxes(weights, 1, 2)
    any_ = pl.BlockSpec(memory_space=pl.ANY)
    vmem = pl.BlockSpec(memory_space=pltpu.VMEM)
    dma = pltpu.SemaphoreType.DMA
    widths = (128, 128, 256)
    return pl.pallas_call(
        kernel,
        out_shape=jax.ShapeDtypeStruct((8, 32, 64), F32),
        in_specs=[any_, any_, vmem, any_],
        out_specs=vmem,
        scratch_shapes=[
            pltpu.VMEM((2, 512, assets), BF16),
            pltpu.VMEM((2, assets, 512), BF16),
            pltpu.VMEM((2, 64, assets), BF16),
            pltpu.VMEM((2, assets, 128), BF16),
            pltpu.VMEM((2, 256, assets), BF16),
            pltpu.VMEM((128, 1024), F32),
            *[pltpu.VMEM((512, w), F32) for w in widths],
            *[pltpu.VMEM((512, w), F32) for w in widths],
            *[pltpu.VMEM((512, w), F32) for w in widths],
            *[pltpu.VMEM((256, w), F32) for w in widths],
            *[pltpu.VMEM((3, 64, w), F32) for w in widths],
            pltpu.VMEM((2, 512, 256), F32),
            pltpu.VMEM((512, 256), F32),
            pltpu.VMEM((7, 64, 256), F32),
            pltpu.VMEM((4, 64, 128), F32),
            pltpu.VMEM((64, 256), F32),
            pltpu.VMEM((64, 256), F32),
            pltpu.VMEM((256, 1024), F32),
            pltpu.VMEM((256, 128), F32),
            pltpu.VMEM((64, 1024), F32),
            pltpu.VMEM((8, 32, 64), F32),
            pltpu.VMEM((8, 32, 64), F32),
            dma((3, 2)), dma((3, 2)), dma((3, 2)), dma((3, 2)), dma((4, 2)), dma((4, 2)),
            dma((2,)), dma((2,)), dma((2,)), dma((2,)), dma((5,)), dma, dma,
            dma((4,)), dma((4,)), dma((3,)), dma((3,)), dma((3, 3)), dma((3, 3)), dma((7,)), dma((7,)),
            dma((4, 7)), dma((4, 7)), dma, dma, dma((8,)), dma((8,)), dma((8,)), dma((8,)),
        ],
        compiler_params=pltpu.CompilerParams(collective_id=0, has_side_effects=True),
    )(loadings, wt, specific, factor_cov)


def solution(mesh):
    in_specs = (P(None, "row", "col"), P(None, "row", "col"), P(None, "row"), P(None, "col", None))
    out_specs = P(None, "row", "col")
    return jax.shard_map(shards, mesh=mesh, in_specs=in_specs, out_specs=out_specs, check_vma=False)
```

```python
import jax
import jax.numpy as jnp
from jax import lax
from jax.experimental import pallas as pl
from jax.experimental.pallas import tpu as pltpu
from jax.sharding import PartitionSpec as P

MESH = pl.DeviceIdType.MESH
F32 = jnp.float32
BF16 = jnp.bfloat16
NT = (((1,), (1,)), ((), ()))
SLOT = {0: 0, 2: 1, 1: 2, 3: 3}
OTHERS = ((2, 1), (1, 1), (3, 1), (2, 0), (1, 0), (3, 0), (0, 1))


def halves(value):
    top = value.astype(BF16)
    return top, (value - top.astype(F32)).astype(BF16)


def dot_nt(a, b):
    (a_top, a_low), (b_top, b_low) = halves(a), halves(b)

    def one(p, q):
        return lax.dot_general(p, q, NT, preferred_element_type=F32)

    return one(a_top, b_top) + (one(a_top, b_low) + one(a_low, b_top))


def kernel(load_ref, wt_ref, spec_ref, fcov_ref, out_ref,
           wt_all, l_all, w_pass, l_pass, wg, f_rows,
           part_o, send_o, got_o, xg_o, zg_o, part_f, send_f, got_f, rs_f,
           part_s, send_s, got_s, zg_s, sum_s, in_s,
           two, got_n, rs_n, red, s_red, s_tile, e_all, left_val, left_buf, obuf, oin,
           wy_s, wy_r, ly_s, ly_r, wx_s, wx_r, wf_s, wf_r, lf_s, lf_r, loc, f_s, f_r,
           cc_s, cc_r, xl_s, xl_r, zz_s, zz_r, rf_s, rf_r, rn_s, rn_r, ag_s, ag_r, sx_s, sx_r, sd_s, sd_r, sl_s, sl_r, sc_s, sc_r,
           la_s, la_r, fo_s, fo_r):
    row, col = lax.axis_index("row"), lax.axis_index("col")
    z, xl, core = row // 4, (row // 2) % 2, row % 2
    y, xh = col // 2, col % 2
    day = 2 * y + core

    def dev(z_, xl_, core_, y_, xh_):
        return (z_ * 4 + xl_ * 2 + core_, y_ * 2 + xh_)

    def remote(src, dst, ssem, rsem, to):
        return pltpu.make_async_remote_copy(
            src_ref=src, dst_ref=dst, send_sem=ssem, recv_sem=rsem,
            device_id=to, device_id_type=MESH)

    def loop(lo, hi, body):
        def step(k, _):
            body(k)
            return 0

        lax.fori_loop(lo, hi, step, 0)

    def part64(i):
        return pl.ds(pl.multiple_of(i * 64, 64), 64)

    def lanes128(i):
        return pl.ds(pl.multiple_of(i * 128, 128), 128)

    def lanes256(i):
        return pl.ds(pl.multiple_of(i * 256, 256), 256)

    bar = pltpu.get_barrier_semaphore()

    def greet(to):
        pl.semaphore_signal(bar, inc=1, device_id=to, device_id_type=MESH)

    def greet_line(k):
        a = (core * 4 + y + k) % 8
        greet(dev(z, xl, a // 4, a % 4, xh))

    def greet_plane(k):
        b = (z * 4 + xl * 2 + xh + k) % 16
        greet(dev(b // 4, (b // 2) % 2, core, y, b % 2))

    def greet_swap(k):
        greet(dev(z, xh, k // 4, k % 4, xl))

    loop(1, 8, greet_line)
    loop(1, 16, greet_plane)

    @pl.when(xl != xh)
    def _():
        loop(0, 8, greet_swap)
        pl.semaphore_wait(bar, 30)

    @pl.when(xl == xh)
    def _():
        pl.semaphore_wait(bar, 22)

    def block_of(b):
        return part64(4 * xh + b)

    here = block_of(y)
    across = dev(z, xl, core, y, 1 - xh)
    near = (1, 3)
    own = []
    wy, wx, ly, wf, lf = {}, {}, {}, {}, {}

    def w_near(dy, dl):
        ty = (y + dy) % 4
        wy[dy, dl] = remote(wt_ref.at[2 * ty + dl], wt_all.at[dl, here, :],
                            wy_s.at[dy - 1, dl], wy_r.at[dy - 1, dl], dev(z, xl, core, ty, xh))
        wy[dy, dl].start()

    def w_across(rel, dl):
        rows = block_of((y + rel) % 4)
        src = wt_ref.at[2 * y + dl] if rel == 0 else wt_all.at[dl, rows, :]
        wx[rel, dl] = remote(src, wt_all.at[dl, rows, :], wx_s.at[rel, dl], wx_r.at[rel, dl], across)
        wx[rel, dl].start()

    def w_arrived(rel, dl):
        wy[4 - rel, dl].wait_recv()
        w_across(rel, dl)

    def l_near(dy, dl):
        ty = (y + dy) % 4
        ly[dy, dl] = remote(load_ref.at[2 * ty + dl], l_all.at[dl, :, pl.ds(128 * SLOT[4 - dy], 128)],
                            ly_s.at[dy - 1, dl], ly_r.at[dy - 1, dl], dev(z, xl, core, ty, xh))
        ly[dy, dl].start()

    for dy in near:
        w_near(dy, 0)
    for dl in range(2):
        w_across(0, dl)
        own.append(pltpu.make_async_copy(wt_ref.at[2 * y + dl], wt_all.at[dl, here, :], loc.at[dl]))
        own[-1].start()
    for dl in range(2):
        wf[dl] = remote(wt_ref.at[2 * ((y + 2) % 4) + dl], w_pass.at[dl], wf_s.at[dl], wf_r.at[dl],
                        dev(z, xl, core, (y + near[dl]) % 4, xh))
        wf[dl].start()
    for dy in near:
        w_near(dy, 1)
    for dl in range(2):
        own.append(pltpu.make_async_copy(load_ref.at[2 * y + dl], l_all.at[dl, :, pl.ds(0, 128)], loc.at[2 + dl]))
        own[-1].start()
    w_arrived(1, 0)
    w_arrived(3, 0)
    for dl in range(2):
        wf[dl].wait_recv()
        wy[2, dl] = remote(w_pass.at[dl], wt_all.at[dl, block_of((y + near[1 - dl]) % 4), :],
                           wy_s.at[1, dl], wy_r.at[1, dl], dev(z, xl, core, (y + near[dl]) % 4, xh))
        wy[2, dl].start()
    for dl in range(2):
        lf[dl] = remote(load_ref.at[2 * ((y + 2) % 4) + dl], l_pass.at[dl], lf_s.at[dl], lf_r.at[dl],
                        dev(z, xl, core, (y + near[dl]) % 4, xh))
        lf[dl].start()
    for dy in near:
        l_near(dy, 0)
    w_arrived(1, 1)
    w_arrived(3, 1)
    w_arrived(2, 0)
    w_arrived(2, 1)
    for c in own:
        c.wait()
    for dl in range(2):
        scale = spec_ref[pl.ds(2 * y + dl, 1), :]
        w = wt_all[dl, lanes256(xh), :]
        wg[dl] = (scale * w.astype(F32)).astype(BF16)
    mate = dev(z, xl, 1 - core, y, xh)
    beside = dev(z, 1 - xl, core, y, xh)
    kept, given = lanes256(xl), lanes256(1 - xl)

    def l_dot(lo, n):
        def product(d):
            return jnp.dot(wt_all[d], l_all[d, :, pl.ds(lo, n)], preferred_element_type=F32)

        return product

    class Group:
        def __init__(self, i, part, send, got, xg, zg, product):
            self.i, self.part, self.send, self.got, self.xg, self.zg = i, part, send, got, xg, zg
            self.product = product
            self.pair = remote(send, got, cc_s.at[i], cc_r.at[i], mate)
            self.side = remote(part.at[given, :], xg, xl_s.at[i], xl_r.at[i], beside)

        def dots(self):
            self.send[...] = self.product(1 - core)
            self.pair.start()
            self.part[...] = self.product(core)

        def over_x(self):
            self.pair.wait_recv()
            self.part[given, :] = self.part[given, :] + self.got[given, :]
            self.side.start()
            self.part[kept, :] = self.part[kept, :] + self.got[kept, :]

        def line(self, k):
            to = (z + k) % 4
            return remote(self.xg.at[part64(to), :], self.zg.at[k - 1],
                          zz_s.at[self.i, k - 1], zz_r.at[self.i, k - 1], dev(to, xl, core, y, xh))

        def over_z(self):
            self.side.wait_recv()
            self.xg[...] = self.xg[...] + self.part[kept, :]
            for k in (1, 3, 2):
                self.line(k).start()

        def total(self):
            for k in (1, 3, 2):
                self.line(k).wait_recv()
            return (self.xg[part64(z), :] + self.zg[0]) + (self.zg[1] + self.zg[2])

        def sent(self):
            self.pair.wait_send()
            self.side.wait_send()
            for k in (1, 3, 2):
                self.line(k).wait_send()

    alike = xl == xh
    differ = xl != xh

    class Specific:
        def __init__(self, i, rows, keep, give):
            self.i, self.rows, self.keep, self.give = i, rows, keep, give
            self.pair = remote(send_s.at[i], got_s.at[i], sc_s.at[i], sc_r.at[i], mate)
            self.side = remote(sum_s.at[i], in_s.at[i], sd_s.at[i], sd_r.at[i], beside)

        def product(self, d):
            return lax.dot_general(wt_all[d, self.rows, :], wg[d], NT, preferred_element_type=F32)

        def dots(self):
            send_s[self.i] = self.product(1 - core)
            self.pair.start()
            part_s[self.i] = self.product(core)

        def line(self, k):
            to = (z + k) % 4
            return remote(part_s.at[self.i, part64(to), :], zg_s.at[self.i, k - 1],
                          sl_s.at[self.i, k - 1], sl_r.at[self.i, k - 1], dev(to, xl, core, y, xh))

        def over_z(self):
            self.pair.wait_recv()
            part_s[self.i] = part_s[self.i] + got_s[self.i]
            for k in (2, 1, 3):
                self.line(k).start()

        def over_x(self):
            for k in (1, 3, 2):
                self.line(k).wait_recv()
            i = self.i
            sum_s[i] = (part_s[i, part64(z), :] + zg_s[i, 0]) + (zg_s[i, 1] + zg_s[i, 2])

            @pl.when(self.give)
            def _():
                self.side.start()

        def total(self):
            self.side.wait_recv()
            return sum_s[self.i] + in_s[self.i]

        def sent(self):
            self.pair.wait_send()
            for k in (1, 3, 2):
                self.line(k).wait_send()

            @pl.when(self.give)
            def _():
                self.side.wait_send()

    g_s = Specific(0, lanes256(xh), alike, differ)
    g_s.dots()
    g_s.over_z()
    for dl in range(2):
        lf[dl].wait_recv()
        ly[2, dl] = remote(l_pass.at[dl], l_all.at[dl, :, pl.ds(128 * SLOT[2], 128)],
                           ly_s.at[1, dl], ly_r.at[1, dl], dev(z, xl, core, (y + near[dl]) % 4, xh))
        ly[2, dl].start()
    for dy in near:
        l_near(dy, 1)
    turn = (z + 2 * core) % 4
    yq = (y + turn) % 4
    yd = (y + 4 - turn) % 4
    f_copy = remote(fcov_ref.at[2 * yd + core], f_rows, f_s, f_r, dev(z, xl, core, yd, xh))
    f_own = pltpu.make_async_copy(fcov_ref.at[day], f_rows, loc.at[4])

    g_s.over_x()
    for dl in range(2):
        for rel in (0, 1, 3, 2):
            wx[rel, dl].wait_recv()
    me_p = 4 * xl + z

    class Straight:
        def __init__(self, i, part, send, got, rs, product):
            self.part, self.send, self.got, self.rs, self.product = part, send, got, rs, product
            self.pair = remote(send, got, cc_s.at[i], cc_r.at[i], mate)

        dots = Group.dots

        def copy(self, k):
            dz, dx = OTHERS[k]
            tz, tx = (z + dz) % 4, (xl + dx) % 2
            return remote(self.part.at[part64(4 * tx + tz), :], self.rs.at[k], rf_s.at[k], rf_r.at[k],
                          dev(tz, tx, core, y, xh))

        def add(self):
            self.pair.wait_recv()
            self.part[...] = self.part[...] + self.got[...]
            for k in range(7):
                self.copy(k).start()

        def total(self):
            for k in range(7):
                self.copy(k).wait_recv()
            total = self.part[part64(me_p), :]
            for k in range(7):
                total = total + self.rs[k]
            return total

        def sent(self):
            self.pair.wait_send()
            for k in range(7):
                self.copy(k).wait_send()

    me8 = 2 * z + xh

    def spread(u, k, block):
        dz, dx = OTHERS[k]
        return remote(red.at[u], e_all.at[part64(z), lanes128(block)], ag_s.at[u, k], ag_r.at[u, k],
                      dev((z + dz) % 4, xl, core, y, (xh + dx) % 2))

    def gather(value, u, rel):
        block = 2 * ((y + rel) % 4) + xh
        red[u] = value
        for k in range(7):
            spread(u, k, block).start()
        e_all[part64(z), lanes128(block)] = value

    def along(u, k, rel):
        dz, _ = OTHERS[k]
        pair = e_all.at[part64(z), lanes256((y + rel) % 4)]
        return remote(pair, pair, ag_s.at[u, k], ag_r.at[u, k], dev((z + dz) % 4, xl, core, y, xh))

    def gather_x(value, u, rel):
        block = 2 * ((y + rel) % 4) + xh
        red[u] = value
        spread(u, 6, block).start()
        e_all[part64(z), lanes128(block)] = value

    def gather_z(u, rel):
        spread(u, 6, 0).wait_recv()
        for k in (3, 4, 5):
            along(u, k, rel).start()

    def gathered(u, rel):
        for k in (3, 4, 5):
            along(u, k, rel).wait_recv()

    def gather_sent(u, rel):
        for k in (3, 4, 5):
            along(u, k, rel).wait_send()
        spread(u, 6, 0).wait_send()

    g_o = Group(0, part_o, send_o, got_o, xg_o, zg_o, l_dot(0, 128))
    g_f = Straight(1, part_f, send_f, got_f, rs_f, l_dot(128, 128))
    g_r = Specific(1, lanes256(1 - xh), differ, alike)


    def pair_n(dl, h):
        half = pl.ds(256 * h, 256)
        return remote(two.at[dl, half, :], got_n.at[half, :], cc_s.at[3 + h], cc_r.at[3 + h], mate)

    def rn(k):
        dz, dx = OTHERS[k]
        tz, tx = (z + dz) % 4, (xl + dx) % 2
        return remote(two.at[core, part64(4 * tx + tz), :], rs_n.at[k], rn_s.at[k], rn_r.at[k],
                      dev(tz, tx, core, y, xh))

    def near_dot(dl):
        for dy in near:
            ly[dy, dl].wait_recv()
        for h in range(2):
            half = pl.ds(256 * h, 256)
            two[dl, half, :] = jnp.dot(wt_all[dl, half, :], l_all[dl, :, pl.ds(256, 256)],
                                       preferred_element_type=F32)

            @pl.when(core != dl)
            def _():
                pair_n(dl, h).start()

    def near_add(dl):
        @pl.when(core == dl)
        def _():
            for h in range(2):
                half = pl.ds(256 * h, 256)
                pair_n(dl, h).wait_recv()
                two[dl, half, :] = two[dl, half, :] + got_n[half, :]
            for k in range(7):
                rn(k).start()

    def near_gather(dl, how):
        @pl.when(core == dl)
        def _():
            for k in range(7):
                rn(k).wait_recv()
            total = two[dl, part64(me_p), :]
            for k in range(7):
                total = total + rs_n[k]
            how(total[:, :128], 2, 1)
            how(total[:, 128:], 3, 3)

    g_o.dots()
    g_o.over_x()
    near_dot(0)
    g_r.dots()
    g_o.over_z()
    near_add(0)
    g_r.over_z()
    for dl in range(2):
        ly[2, dl].wait_recv()
    g_f.dots()
    gather_x(g_o.total(), 0, 0)
    g_f.add()
    near_gather(0, gather_x)
    gather_z(0, 0)
    for c in [*wy.values(), *wx.values(), *wf.values()]:
        c.wait_send()
    g_r.over_x()

    @pl.when(core == 0)
    def _():
        gather_z(2, 1)
        gather_z(3, 3)

    gather(g_f.total(), 1, 2)
    near_dot(1)
    @pl.when(turn == 0)
    def _():
        f_own.start()

    @pl.when(turn != 0)
    def _():
        f_copy.start()

    near_add(1)
    near_gather(1, gather)

    @pl.when(turn == 0)
    def _():
        f_own.wait()

    @pl.when(turn != 0)
    def _():
        f_copy.wait_recv()

    def left_part(rel):
        at = lanes256((y + rel) % 4)
        return dot_nt(e_all[:, at], f_rows[:, at])

    gathered(0, 0)
    for k in range(7):
        spread(1, k, 0).wait_recv()
    left_val[...] = left_part(0) + left_part(2)
    g_o.sent()
    g_f.sent()

    @pl.when(core == 0)
    def _():
        gathered(2, 1)
        gathered(3, 3)

    @pl.when(core == 1)
    def _():
        for k in range(7):
            spread(2, k, 0).wait_recv()
            spread(3, k, 0).wait_recv()

    left_val[...] += left_part(1) + left_part(3)

    def la(j):
        return remote(left_val.at[part64(j // 2), :], left_buf.at[:, lanes128(2 * yq + xh)],
                      la_s.at[j], la_r.at[me8], dev(j // 2, j % 2, core, y, xl))

    me_t = 2 * z + xl

    def unless(skip, body):
        @pl.when(jnp.logical_not(skip))
        def _():
            body()

    loop(0, 8, lambda j: unless(jnp.logical_and(alike, j == me_t), lambda: la(j).start()))

    @pl.when(alike)
    def _():
        left_buf[:, lanes128(2 * yq + xh)] = left_val[part64(z), :]

    swap = remote(s_red, s_tile, sx_s, sx_r, dev(z, xh, core, y, xl))

    @pl.when(alike)
    def _():
        s_tile[...] = g_s.total()

    @pl.when(differ)
    def _():
        s_red[...] = g_r.total()
        swap.start()

    g_s.sent()
    g_r.sent()
    gather_sent(0, 0)
    for k in range(7):
        spread(1, k, 0).wait_send()

    @pl.when(core == 0)
    def _():
        gather_sent(2, 1)
        gather_sent(3, 3)

    @pl.when(core == 1)
    def _():
        for k in range(7):
            spread(2, k, 0).wait_send()
            spread(3, k, 0).wait_send()

    for k in range(7):
        rn(k).wait_send()

    def la_in(j):
        return remote(left_val.at[part64(0), :], left_buf.at[:, lanes128(0)], la_s.at[0], la_r.at[j], mate)

    loop(0, 8, lambda j: unless(jnp.logical_and(alike, j == me8), lambda: la_in(j).wait_recv()))
    tile = dot_nt(left_buf[...], e_all[...])

    @pl.when(xl != xh)
    def _():
        swap.wait_recv()

    tile = tile + s_tile[...]
    for h in range(2):
        for b in range(4):
            obuf[4 * h + b] = tile[32 * h:32 * h + 32, 64 * b:64 * b + 64]

    def fo(i):
        return remote(obuf.at[i], oin.at[day], fo_s.at[i], fo_r.at[day], dev(z, xh, i // 4, i % 4, xl))

    me_o = 4 * core + y
    loop(0, 8, lambda i: unless(jnp.logical_and(alike, i == me_o), lambda: fo(i).start()))

    @pl.when(alike)
    def _():
        oin[day] = obuf[me_o]

    for c in [*ly.values(), *lf.values()]:
        c.wait_send()
    for h in range(2):
        pair_n(1 - core, h).wait_send()

    @pl.when(xl != xh)
    def _():
        swap.wait_send()

    @pl.when(turn != 0)
    def _():
        f_copy.wait_send()

    loop(0, 8, lambda j: unless(jnp.logical_and(alike, j == me_t), lambda: la(j).wait_send()))

    def fo_in(d):
        return remote(obuf.at[0], oin.at[d], fo_s.at[0], fo_r.at[d], mate)

    loop(0, 8, lambda d: unless(jnp.logical_and(alike, d == day), lambda: fo_in(d).wait_recv()))
    out_ref[...] = oin[...]
    loop(0, 8, lambda i: unless(jnp.logical_and(alike, i == me_o), lambda: fo(i).wait_send()))


def shards(loadings, weights, specific, factor_cov):
    assets = loadings.shape[1]
    wt = jnp.swapaxes(weights, 1, 2)
    any_ = pl.BlockSpec(memory_space=pl.ANY)
    vmem = pl.BlockSpec(memory_space=pltpu.VMEM)
    dma = pltpu.SemaphoreType.DMA
    return pl.pallas_call(
        kernel,
        out_shape=jax.ShapeDtypeStruct((8, 32, 64), F32),
        in_specs=[any_, any_, vmem, any_],
        out_specs=vmem,
        scratch_shapes=[
            pltpu.VMEM((2, 512, assets), BF16),
            pltpu.VMEM((2, assets, 512), BF16),
            pltpu.VMEM((2, 64, assets), BF16),
            pltpu.VMEM((2, assets, 128), BF16),
            pltpu.VMEM((2, 256, assets), BF16),
            pltpu.VMEM((128, 1024), F32),
            *[pltpu.VMEM((512, 128), F32)] * 3,
            pltpu.VMEM((256, 128), F32),
            pltpu.VMEM((3, 64, 128), F32),
            *[pltpu.VMEM((512, 128), F32)] * 3,
            pltpu.VMEM((7, 64, 128), F32),
            *[pltpu.VMEM((2, 256, 256), F32)] * 3,
            pltpu.VMEM((2, 3, 64, 256), F32),
            pltpu.VMEM((2, 64, 256), F32),
            pltpu.VMEM((2, 64, 256), F32),
            pltpu.VMEM((2, 512, 256), F32),
            pltpu.VMEM((512, 256), F32),
            pltpu.VMEM((7, 64, 256), F32),
            pltpu.VMEM((4, 64, 128), F32),
            pltpu.VMEM((64, 256), F32),
            pltpu.VMEM((64, 256), F32),
            pltpu.VMEM((256, 1024), F32),
            pltpu.VMEM((256, 128), F32),
            pltpu.VMEM((64, 1024), F32),
            pltpu.VMEM((8, 32, 64), F32),
            pltpu.VMEM((8, 32, 64), F32),
            dma((3, 2)), dma((3, 2)), dma((3, 2)), dma((3, 2)), dma((4, 2)), dma((4, 2)),
            dma((2,)), dma((2,)), dma((2,)), dma((2,)), dma((5,)), dma, dma,
            dma((5,)), dma((5,)), dma((3,)), dma((3,)), dma((3, 3)), dma((3, 3)), dma((7,)), dma((7,)), dma((7,)), dma((7,)),
            dma((4, 7)), dma((4, 7)), dma, dma,
            dma((2,)), dma((2,)), dma((2, 3)), dma((2, 3)), dma((2,)), dma((2,)), dma((8,)), dma((8,)), dma((8,)), dma((8,)),
        ],
        compiler_params=pltpu.CompilerParams(collective_id=0, has_side_effects=True),
    )(loadings, wt, specific, factor_cov)


def solution(mesh):
    in_specs = (P(None, "row", "col"), P(None, "row", "col"), P(None, "row"), P(None, "col", None))
    out_specs = P(None, "row", "col")
    return jax.shard_map(shards, mesh=mesh, in_specs=in_specs, out_specs=out_specs, check_vma=False)
```

```python
import jax
import jax.numpy as jnp
from jax import lax
from jax.experimental import pallas as pl
from jax.experimental.pallas import tpu as pltpu
from jax.sharding import PartitionSpec as P

MESH = pl.DeviceIdType.MESH
F32 = jnp.float32
BF16 = jnp.bfloat16
NT = (((1,), (1,)), ((), ()))
SLOT = {0: 0, 2: 1, 1: 2, 3: 3}
OTHERS = ((2, 1), (1, 1), (3, 1), (2, 0), (1, 0), (3, 0), (0, 1))


def halves(value):
    top = value.astype(BF16)
    return top, (value - top.astype(F32)).astype(BF16)


def dot_nt(a, b):
    (a_top, a_low), (b_top, b_low) = halves(a), halves(b)

    def one(p, q):
        return lax.dot_general(p, q, NT, preferred_element_type=F32)

    return one(a_top, b_top) + (one(a_top, b_low) + one(a_low, b_top))


def kernel(load_ref, wt_ref, spec_ref, fcov_ref, out_ref,
           wt_all, l_all, w_pass, l_pass, spec, wg, f_rows,
           part_o, send_o, got_o, xg_o, zg_o, part_f, send_f, got_f, rs_f,
           part_s, send_s, got_s, zg_s, sum_s, in_s,
           two, got_n, rs_n, red, s_red, s_tile, e_all, left_val, left_buf, obuf,
           wy_s, wy_r, ly_s, ly_r, wx_s, wx_r, wf_s, wf_r, lf_s, lf_r, loc, f_s, f_r,
           cc_s, cc_r, xl_s, xl_r, zz_s, zz_r, rf_s, rf_r, rn_s, rn_r, ag_s, ag_r, sx_s, sx_r, sd_s, sd_r, sl_s, sl_r, sc_s, sc_r,
           la_s, la_r, fo_s, fo_r):
    row, col = lax.axis_index("row"), lax.axis_index("col")
    z, xl, core = row // 4, (row // 2) % 2, row % 2
    y, xh = col // 2, col % 2
    day = 2 * y + core

    def dev(z_, xl_, core_, y_, xh_):
        return (z_ * 4 + xl_ * 2 + core_, y_ * 2 + xh_)

    def remote(src, dst, ssem, rsem, to):
        return pltpu.make_async_remote_copy(
            src_ref=src, dst_ref=dst, send_sem=ssem, recv_sem=rsem,
            device_id=to, device_id_type=MESH)

    def loop(lo, hi, body):
        def step(k, _):
            body(k)
            return 0

        lax.fori_loop(lo, hi, step, 0)

    def part64(i):
        return pl.ds(pl.multiple_of(i * 64, 64), 64)

    def lanes128(i):
        return pl.ds(pl.multiple_of(i * 128, 128), 128)

    def lanes256(i):
        return pl.ds(pl.multiple_of(i * 256, 256), 256)

    bar = pltpu.get_barrier_semaphore()

    def greet(to):
        pl.semaphore_signal(bar, inc=1, device_id=to, device_id_type=MESH)

    for k in (1, 2, 3):
        greet(dev((z + k) % 4, xl, core, y, xh))
    for k in (1, 3):
        greet(dev(z, xl, core, (y + k) % 4, xh))
    greet(dev(z, 1 - xl, core, y, xh))
    greet(dev(z, xl, core, y, 1 - xh))
    greet(dev(z, xl, 1 - core, y, xh))
    pl.semaphore_wait(bar, 8)

    def block_of(b):
        return part64(4 * xh + b)

    here = block_of(y)
    across = dev(z, xl, core, y, 1 - xh)
    near = (1, 3)
    own = []
    wy, wx, ly, wf, lf = {}, {}, {}, {}, {}

    def w_near(dy, dl):
        ty = (y + dy) % 4
        wy[dy, dl] = remote(wt_ref.at[2 * ty + dl], wt_all.at[dl, here, :],
                            wy_s.at[dy - 1, dl], wy_r.at[dy - 1, dl], dev(z, xl, core, ty, xh))
        wy[dy, dl].start()

    def w_across(rel, dl):
        rows = block_of((y + rel) % 4)
        src = wt_ref.at[2 * y + dl] if rel == 0 else wt_all.at[dl, rows, :]
        wx[rel, dl] = remote(src, wt_all.at[dl, rows, :], wx_s.at[rel, dl], wx_r.at[rel, dl], across)
        wx[rel, dl].start()

    def w_arrived(rel, dl):
        wy[4 - rel, dl].wait_recv()
        w_across(rel, dl)

    def l_near(dy, dl):
        ty = (y + dy) % 4
        ly[dy, dl] = remote(load_ref.at[2 * ty + dl], l_all.at[dl, :, pl.ds(128 * SLOT[4 - dy], 128)],
                            ly_s.at[dy - 1, dl], ly_r.at[dy - 1, dl], dev(z, xl, core, ty, xh))
        ly[dy, dl].start()

    for dy in near:
        w_near(dy, 0)
    for dl in range(2):
        w_across(0, dl)
        own.append(pltpu.make_async_copy(wt_ref.at[2 * y + dl], wt_all.at[dl, here, :], loc.at[dl]))
        own[-1].start()
    for dl in range(2):
        wf[dl] = remote(wt_ref.at[2 * ((y + 2) % 4) + dl], w_pass.at[dl], wf_s.at[dl], wf_r.at[dl],
                        dev(z, xl, core, (y + near[dl]) % 4, xh))
        wf[dl].start()
    for dy in near:
        w_near(dy, 1)
    for dl in range(2):
        own.append(pltpu.make_async_copy(load_ref.at[2 * y + dl], l_all.at[dl, :, pl.ds(0, 128)], loc.at[2 + dl]))
        own[-1].start()
    own.append(pltpu.make_async_copy(spec_ref, spec, loc.at[5]))
    own[-1].start()
    w_arrived(1, 0)
    w_arrived(3, 0)
    for dl in range(2):
        wf[dl].wait_recv()
        wy[2, dl] = remote(w_pass.at[dl], wt_all.at[dl, block_of((y + near[1 - dl]) % 4), :],
                           wy_s.at[1, dl], wy_r.at[1, dl], dev(z, xl, core, (y + near[dl]) % 4, xh))
        wy[2, dl].start()
    for dl in range(2):
        lf[dl] = remote(load_ref.at[2 * ((y + 2) % 4) + dl], l_pass.at[dl], lf_s.at[dl], lf_r.at[dl],
                        dev(z, xl, core, (y + near[dl]) % 4, xh))
        lf[dl].start()
    for dy in near:
        l_near(dy, 0)
    w_arrived(1, 1)
    w_arrived(3, 1)
    w_arrived(2, 0)
    w_arrived(2, 1)
    for c in own:
        c.wait()
    for dl in range(2):
        scale = spec[pl.ds(2 * y + dl, 1), :]
        w = wt_all[dl, lanes256(xh), :]
        wg[dl] = (scale * w.astype(F32)).astype(BF16)
    mate = dev(z, xl, 1 - core, y, xh)
    beside = dev(z, 1 - xl, core, y, xh)
    kept, given = lanes256(xl), lanes256(1 - xl)

    def l_dot(lo, n):
        def product(d):
            return jnp.dot(wt_all[d], l_all[d, :, pl.ds(lo, n)], preferred_element_type=F32)

        return product

    class Group:
        def __init__(self, i, part, send, got, xg, zg, product):
            self.i, self.part, self.send, self.got, self.xg, self.zg = i, part, send, got, xg, zg
            self.product = product
            self.pair = remote(send, got, cc_s.at[i], cc_r.at[i], mate)
            self.side = remote(part.at[given, :], xg, xl_s.at[i], xl_r.at[i], beside)

        def dots(self):
            self.send[...] = self.product(1 - core)
            self.pair.start()
            self.part[...] = self.product(core)

        def over_x(self):
            self.pair.wait_recv()
            self.part[given, :] = self.part[given, :] + self.got[given, :]
            self.side.start()
            self.part[kept, :] = self.part[kept, :] + self.got[kept, :]

        def line(self, k):
            to = (z + k) % 4
            return remote(self.xg.at[part64(to), :], self.zg.at[k - 1],
                          zz_s.at[self.i, k - 1], zz_r.at[self.i, k - 1], dev(to, xl, core, y, xh))

        def over_z(self):
            self.side.wait_recv()
            self.xg[...] = self.xg[...] + self.part[kept, :]
            for k in (1, 3, 2):
                self.line(k).start()

        def total(self):
            for k in (1, 3, 2):
                self.line(k).wait_recv()
            return (self.xg[part64(z), :] + self.zg[0]) + (self.zg[1] + self.zg[2])

        def sent(self):
            self.pair.wait_send()
            self.side.wait_send()
            for k in (1, 3, 2):
                self.line(k).wait_send()

    alike = xl == xh
    differ = xl != xh

    class Specific:
        def __init__(self, i, rows, keep, give):
            self.i, self.rows, self.keep, self.give = i, rows, keep, give
            self.pair = remote(send_s.at[i], got_s.at[i], sc_s.at[i], sc_r.at[i], mate)
            self.side = remote(sum_s.at[i], in_s.at[i], sd_s.at[i], sd_r.at[i], beside)

        def product(self, d):
            return lax.dot_general(wt_all[d, self.rows, :], wg[d], NT, preferred_element_type=F32)

        def dots(self):
            send_s[self.i] = self.product(1 - core)
            self.pair.start()
            part_s[self.i] = self.product(core)

        def line(self, k):
            to = (z + k) % 4
            return remote(part_s.at[self.i, part64(to), :], zg_s.at[self.i, k - 1],
                          sl_s.at[self.i, k - 1], sl_r.at[self.i, k - 1], dev(to, xl, core, y, xh))

        def over_z(self):
            self.pair.wait_recv()
            part_s[self.i] = part_s[self.i] + got_s[self.i]
            for k in (2, 1, 3):
                self.line(k).start()

        def over_x(self):
            for k in (1, 3, 2):
                self.line(k).wait_recv()
            i = self.i
            sum_s[i] = (part_s[i, part64(z), :] + zg_s[i, 0]) + (zg_s[i, 1] + zg_s[i, 2])

            @pl.when(self.give)
            def _():
                self.side.start()

        def total(self):
            self.side.wait_recv()
            return sum_s[self.i] + in_s[self.i]

        def sent(self):
            self.pair.wait_send()
            for k in (1, 3, 2):
                self.line(k).wait_send()

            @pl.when(self.give)
            def _():
                self.side.wait_send()

    g_s = Specific(0, lanes256(xh), alike, differ)
    g_s.dots()
    g_s.over_z()
    for dl in range(2):
        lf[dl].wait_recv()
        ly[2, dl] = remote(l_pass.at[dl], l_all.at[dl, :, pl.ds(128 * SLOT[2], 128)],
                           ly_s.at[1, dl], ly_r.at[1, dl], dev(z, xl, core, (y + near[dl]) % 4, xh))
        ly[2, dl].start()
    for dy in near:
        l_near(dy, 1)
    turn = (z + 2 * core) % 4
    yq = (y + turn) % 4
    yd = (y + 4 - turn) % 4
    f_copy = remote(fcov_ref.at[2 * yd + core], f_rows, f_s, f_r, dev(z, xl, core, yd, xh))
    f_own = pltpu.make_async_copy(fcov_ref.at[day], f_rows, loc.at[4])

    g_s.over_x()
    for dl in range(2):
        for rel in (0, 1, 3, 2):
            wx[rel, dl].wait_recv()
    me_p = 4 * xl + z

    class Straight:
        def __init__(self, i, part, send, got, rs, product):
            self.part, self.send, self.got, self.rs, self.product = part, send, got, rs, product
            self.pair = remote(send, got, cc_s.at[i], cc_r.at[i], mate)

        dots = Group.dots

        def copy(self, k):
            dz, dx = OTHERS[k]
            tz, tx = (z + dz) % 4, (xl + dx) % 2
            return remote(self.part.at[part64(4 * tx + tz), :], self.rs.at[k], rf_s.at[k], rf_r.at[k],
                          dev(tz, tx, core, y, xh))

        def add(self):
            self.pair.wait_recv()
            self.part[...] = self.part[...] + self.got[...]
            for k in range(7):
                self.copy(k).start()

        def total(self):
            for k in range(7):
                self.copy(k).wait_recv()
            total = self.part[part64(me_p), :]
            for k in range(7):
                total = total + self.rs[k]
            return total

        def sent(self):
            self.pair.wait_send()
            for k in range(7):
                self.copy(k).wait_send()

    me8 = 2 * z + xh

    def spread(u, k, block):
        dz, dx = OTHERS[k]
        return remote(red.at[u], e_all.at[part64(z), lanes128(block)], ag_s.at[u, k], ag_r.at[u, k],
                      dev((z + dz) % 4, xl, core, y, (xh + dx) % 2))

    def gather(value, u, rel):
        block = 2 * ((y + rel) % 4) + xh
        red[u] = value
        for k in range(7):
            spread(u, k, block).start()
        e_all[part64(z), lanes128(block)] = value

    def along(u, k, rel):
        dz, _ = OTHERS[k]
        pair = e_all.at[part64(z), lanes256((y + rel) % 4)]
        return remote(pair, pair, ag_s.at[u, k], ag_r.at[u, k], dev((z + dz) % 4, xl, core, y, xh))

    def gather_x(value, u, rel):
        block = 2 * ((y + rel) % 4) + xh
        red[u] = value
        spread(u, 6, block).start()
        e_all[part64(z), lanes128(block)] = value

    def gather_z(u, rel):
        spread(u, 6, 0).wait_recv()
        for k in (3, 4, 5):
            along(u, k, rel).start()

    def gathered(u, rel):
        for k in (3, 4, 5):
            along(u, k, rel).wait_recv()

    def gather_sent(u, rel):
        for k in (3, 4, 5):
            along(u, k, rel).wait_send()
        spread(u, 6, 0).wait_send()

    g_o = Group(0, part_o, send_o, got_o, xg_o, zg_o, l_dot(0, 128))
    g_f = Straight(1, part_f, send_f, got_f, rs_f, l_dot(128, 128))
    g_r = Specific(1, lanes256(1 - xh), differ, alike)


    def pair_n(dl, h):
        half = (given, kept)[h]
        return remote(two.at[dl, half, :], got_n.at[half, :], cc_s.at[3 + h], cc_r.at[3 + h], mate)

    def rn(k):
        dz, dx = OTHERS[k]
        tz, tx = (z + dz) % 4, (xl + dx) % 2
        return remote(two.at[core, part64(4 * tx + tz), :], rs_n.at[k], rn_s.at[k], rn_r.at[k],
                      dev(tz, tx, core, y, xh))

    def near_dot(dl):
        for dy in near:
            ly[dy, dl].wait_recv()
        for h, half in enumerate((given, kept)):
            two[dl, half, :] = jnp.dot(wt_all[dl, half, :], l_all[dl, :, pl.ds(256, 256)],
                                       preferred_element_type=F32)

            @pl.when(core != dl)
            def _():
                pair_n(dl, h).start()

    def near_add(dl):
        @pl.when(core == dl)
        def _():
            for h, half in enumerate((given, kept)):
                pair_n(dl, h).wait_recv()
                two[dl, half, :] = two[dl, half, :] + got_n[half, :]
                for k in range(7):
                    if OTHERS[k][1] == 1 - h:
                        rn(k).start()

    def near_gather(dl, how):
        @pl.when(core == dl)
        def _():
            for k in range(7):
                rn(k).wait_recv()
            total = two[dl, part64(me_p), :]
            for k in range(7):
                total = total + rs_n[k]
            how(total[:, :128], 2, 1)
            how(total[:, 128:], 3, 3)

    g_o.dots()
    g_o.over_x()
    near_dot(0)
    g_r.dots()
    g_o.over_z()
    near_add(0)
    g_r.over_z()
    for dl in range(2):
        ly[2, dl].wait_recv()
    g_f.dots()
    gather_x(g_o.total(), 0, 0)
    g_f.add()
    near_gather(0, gather_x)
    gather_z(0, 0)
    for c in [*wy.values(), *wx.values(), *wf.values()]:
        c.wait_send()
    g_r.over_x()

    @pl.when(core == 0)
    def _():
        gather_z(2, 1)
        gather_z(3, 3)

    gather(g_f.total(), 1, 2)
    near_dot(1)
    @pl.when(turn == 0)
    def _():
        f_own.start()

    @pl.when(turn != 0)
    def _():
        f_copy.start()

    near_add(1)
    near_gather(1, gather)

    @pl.when(turn == 0)
    def _():
        f_own.wait()

    @pl.when(turn != 0)
    def _():
        f_copy.wait_recv()

    def left_part(rel):
        at = lanes256((y + rel) % 4)
        return dot_nt(e_all[:, at], f_rows[:, at])

    gathered(0, 0)
    for k in range(7):
        spread(1, k, 0).wait_recv()
    left_val[...] = left_part(0) + left_part(2)
    g_o.sent()
    g_f.sent()

    @pl.when(core == 0)
    def _():
        gathered(2, 1)
        gathered(3, 3)

    @pl.when(core == 1)
    def _():
        for k in range(7):
            spread(2, k, 0).wait_recv()
            spread(3, k, 0).wait_recv()

    left_val[...] += left_part(1) + left_part(3)

    def la(j):
        return remote(left_val.at[part64(j // 2), :], left_buf.at[:, lanes128(2 * yq + xh)],
                      la_s.at[j], la_r.at[me8], dev(j // 2, j % 2, core, y, xl))

    me_t = 2 * z + xl

    def unless(skip, body):
        @pl.when(jnp.logical_not(skip))
        def _():
            body()

    loop(0, 8, lambda j: unless(jnp.logical_and(alike, j == me_t), lambda: la(j).start()))

    @pl.when(alike)
    def _():
        left_buf[:, lanes128(2 * yq + xh)] = left_val[part64(z), :]

    swap = remote(s_red, s_tile, sx_s, sx_r, dev(z, xh, core, y, xl))

    @pl.when(alike)
    def _():
        s_tile[...] = g_s.total()

    @pl.when(differ)
    def _():
        s_red[...] = g_r.total()
        swap.start()

    g_s.sent()
    g_r.sent()
    gather_sent(0, 0)
    for k in range(7):
        spread(1, k, 0).wait_send()

    @pl.when(core == 0)
    def _():
        gather_sent(2, 1)
        gather_sent(3, 3)

    @pl.when(core == 1)
    def _():
        for k in range(7):
            spread(2, k, 0).wait_send()
            spread(3, k, 0).wait_send()

    for k in range(7):
        rn(k).wait_send()

    def la_in(j):
        return remote(left_val.at[part64(0), :], left_buf.at[:, lanes128(0)], la_s.at[0], la_r.at[j], mate)

    loop(0, 8, lambda j: unless(jnp.logical_and(alike, j == me8), lambda: la_in(j).wait_recv()))
    tile = dot_nt(left_buf[...], e_all[...])

    @pl.when(xl != xh)
    def _():
        swap.wait_recv()

    tile = tile + s_tile[...]
    for h in range(2):
        for b in range(4):
            obuf[4 * h + b] = tile[32 * h:32 * h + 32, 64 * b:64 * b + 64]

    def fo(i):
        return remote(obuf.at[i], out_ref.at[day], fo_s.at[i], fo_r.at[day], dev(z, xh, i // 4, i % 4, xl))

    me_o = 4 * core + y
    stay = pltpu.make_async_copy(obuf.at[me_o], out_ref.at[day], loc.at[6])
    loop(0, 8, lambda i: unless(jnp.logical_and(alike, i == me_o), lambda: fo(i).start()))

    @pl.when(alike)
    def _():
        stay.start()

    for c in [*ly.values(), *lf.values()]:
        c.wait_send()
    for h in range(2):
        pair_n(1 - core, h).wait_send()

    @pl.when(xl != xh)
    def _():
        swap.wait_send()

    @pl.when(turn != 0)
    def _():
        f_copy.wait_send()

    loop(0, 8, lambda j: unless(jnp.logical_and(alike, j == me_t), lambda: la(j).wait_send()))

    def fo_in(d):
        return remote(obuf.at[0], out_ref.at[d], fo_s.at[0], fo_r.at[d], mate)

    loop(0, 8, lambda d: unless(jnp.logical_and(alike, d == day), lambda: fo_in(d).wait_recv()))

    @pl.when(alike)
    def _():
        stay.wait()

    loop(0, 8, lambda i: unless(jnp.logical_and(alike, i == me_o), lambda: fo(i).wait_send()))


def shards(loadings, weights, specific, factor_cov):
    assets = loadings.shape[1]
    wt = jnp.swapaxes(weights, 1, 2)
    any_ = pl.BlockSpec(memory_space=pl.ANY)
    dma = pltpu.SemaphoreType.DMA
    return pl.pallas_call(
        kernel,
        out_shape=jax.ShapeDtypeStruct((8, 32, 64), F32),
        in_specs=[any_] * 4,
        out_specs=any_,
        scratch_shapes=[
            pltpu.VMEM((2, 512, assets), BF16),
            pltpu.VMEM((2, assets, 512), BF16),
            pltpu.VMEM((2, 64, assets), BF16),
            pltpu.VMEM((2, assets, 128), BF16),
            pltpu.VMEM((8, assets), F32),
            pltpu.VMEM((2, 256, assets), BF16),
            pltpu.VMEM((128, 1024), F32),
            *[pltpu.VMEM((512, 128), F32)] * 3,
            pltpu.VMEM((256, 128), F32),
            pltpu.VMEM((3, 64, 128), F32),
            *[pltpu.VMEM((512, 128), F32)] * 3,
            pltpu.VMEM((7, 64, 128), F32),
            *[pltpu.VMEM((2, 256, 256), F32)] * 3,
            pltpu.VMEM((2, 3, 64, 256), F32),
            pltpu.VMEM((2, 64, 256), F32),
            pltpu.VMEM((2, 64, 256), F32),
            pltpu.VMEM((2, 512, 256), F32),
            pltpu.VMEM((512, 256), F32),
            pltpu.VMEM((7, 64, 256), F32),
            pltpu.VMEM((4, 64, 128), F32),
            pltpu.VMEM((64, 256), F32),
            pltpu.VMEM((64, 256), F32),
            pltpu.VMEM((256, 1024), F32),
            pltpu.VMEM((256, 128), F32),
            pltpu.VMEM((64, 1024), F32),
            pltpu.VMEM((8, 32, 64), F32),
            dma((3, 2)), dma((3, 2)), dma((3, 2)), dma((3, 2)), dma((4, 2)), dma((4, 2)),
            dma((2,)), dma((2,)), dma((2,)), dma((2,)), dma((7,)), dma, dma,
            dma((5,)), dma((5,)), dma((3,)), dma((3,)), dma((3, 3)), dma((3, 3)), dma((7,)), dma((7,)), dma((7,)), dma((7,)),
            dma((4, 7)), dma((4, 7)), dma, dma,
            dma((2,)), dma((2,)), dma((2, 3)), dma((2, 3)), dma((2,)), dma((2,)), dma((8,)), dma((8,)), dma((8,)), dma((8,)),
        ],
        compiler_params=pltpu.CompilerParams(collective_id=0, has_side_effects=True),
    )(loadings, wt, specific, factor_cov)


def solution(mesh):
    in_specs = (P(None, "row", "col"), P(None, "row", "col"), P(None, "row"), P(None, "col", None))
    out_specs = P(None, "row", "col")
    return jax.shard_map(shards, mesh=mesh, in_specs=in_specs, out_specs=out_specs, check_vma=False)
```

```python
import jax
import jax.numpy as jnp
from jax import lax
from jax.experimental import pallas as pl
from jax.experimental.pallas import tpu as pltpu
from jax.sharding import PartitionSpec as P

MESH = pl.DeviceIdType.MESH
F32 = jnp.float32
BF16 = jnp.bfloat16
NT = (((1,), (1,)), ((), ()))
SLOT = {0: 0, 2: 1, 1: 2, 3: 3}
OTHERS = ((2, 1), (1, 1), (3, 1), (2, 0), (1, 0), (3, 0), (0, 1))


def halves(value):
    top = value.astype(BF16)
    return top, (value - top.astype(F32)).astype(BF16)


def dot_nt(a, b):
    (a_top, a_low), (b_top, b_low) = halves(a), halves(b)

    def one(p, q):
        return lax.dot_general(p, q, NT, preferred_element_type=F32)

    return one(a_top, b_top) + (one(a_top, b_low) + one(a_low, b_top))


def kernel(load_ref, wt_ref, spec_ref, fcov_ref, out_ref,
           wt_all, l_all, w_pass, l_pass, spec, wg, f_rows,
           part_o, send_o, got_o, xg_o, zg_o, part_f, send_f, got_f, rs_f,
           part_s, send_s, got_s, zg_s, sum_s, in_s,
           two, got_n, rs_n, red, s_red, s_tile, e_all, left_val, left_buf, obuf,
           wy_s, wy_r, ly_s, ly_r, wx_s, wx_r, wf_s, wf_r, lf_s, lf_r, loc, f_s, f_r,
           cc_s, cc_r, xl_s, xl_r, zz_s, zz_r, rf_s, rf_r, rn_s, rn_r, ag_s, ag_r, sx_s, sx_r, sd_s, sd_r, sl_s, sl_r, sc_s, sc_r,
           la_s, la_r, fo_s, fo_r):
    row, col = lax.axis_index("row"), lax.axis_index("col")
    z, xl, core = row // 4, (row // 2) % 2, row % 2
    y, xh = col // 2, col % 2
    day = 2 * y + core

    def dev(z_, xl_, core_, y_, xh_):
        return (z_ * 4 + xl_ * 2 + core_, y_ * 2 + xh_)

    def remote(src, dst, ssem, rsem, to):
        return pltpu.make_async_remote_copy(
            src_ref=src, dst_ref=dst, send_sem=ssem, recv_sem=rsem,
            device_id=to, device_id_type=MESH)

    def loop(lo, hi, body):
        def step(k, _):
            body(k)
            return 0

        lax.fori_loop(lo, hi, step, 0)

    def part64(i):
        return pl.ds(pl.multiple_of(i * 64, 64), 64)

    def lanes128(i):
        return pl.ds(pl.multiple_of(i * 128, 128), 128)

    def lanes256(i):
        return pl.ds(pl.multiple_of(i * 256, 256), 256)

    bar = pltpu.get_barrier_semaphore()

    def greet(to):
        pl.semaphore_signal(bar, inc=1, device_id=to, device_id_type=MESH)

    for k in (1, 2, 3):
        greet(dev((z + k) % 4, xl, core, y, xh))
    for k in (1, 3):
        greet(dev(z, xl, core, (y + k) % 4, xh))
    greet(dev(z, 1 - xl, core, y, xh))
    greet(dev(z, xl, core, y, 1 - xh))
    greet(dev(z, xl, 1 - core, y, xh))
    pl.semaphore_wait(bar, 8)

    def block_of(b):
        return part64(4 * xh + b)

    here = block_of(y)
    across = dev(z, xl, core, y, 1 - xh)
    near = (1, 3)
    assets = l_all.shape[1]
    most, rest = pl.ds(0, 3 * assets // 4), pl.ds(3 * assets // 4, assets // 4)
    own = []
    wy, wx, ly, wf, lf = {}, {}, {}, {}, {}

    def w_near(dy, dl):
        ty = (y + dy) % 4
        wy[dy, dl] = remote(wt_ref.at[2 * ty + dl], wt_all.at[dl, here, :],
                            wy_s.at[dy - 1, dl], wy_r.at[dy - 1, dl], dev(z, xl, core, ty, xh))
        wy[dy, dl].start()

    def w_across(rel, dl):
        rows = block_of((y + rel) % 4)
        src = wt_ref.at[2 * y + dl] if rel == 0 else wt_all.at[dl, rows, :]
        wx[rel, dl] = remote(src, wt_all.at[dl, rows, :], wx_s.at[rel, dl], wx_r.at[rel, dl], across)
        wx[rel, dl].start()

    def w_arrived(rel, dl):
        wy[4 - rel, dl].wait_recv()
        w_across(rel, dl)

    def l_near(dy, dl):
        ty = (y + dy) % 4
        slot = pl.ds(128 * SLOT[4 - dy], 128)
        to = dev(z, xl, core, ty, xh)
        if dl == 0:
            ly[dy, dl] = remote(load_ref.at[2 * ty], l_all.at[0, :, slot],
                                ly_s.at[dy - 1, 0], ly_r.at[dy - 1, 0], to)
            ly[dy, dl].start()
            return
        for rows, i in ((most, 1), (rest, 2)):
            ly[dy, i] = remote(load_ref.at[2 * ty + 1, rows, :], l_all.at[1, rows, slot],
                               ly_s.at[dy - 1, i], ly_r.at[dy - 1, i], to)
            ly[dy, i].start()

    for dy in near:
        w_near(dy, 0)
    for dl in range(2):
        w_across(0, dl)
        own.append(pltpu.make_async_copy(wt_ref.at[2 * y + dl], wt_all.at[dl, here, :], loc.at[dl]))
        own[-1].start()
    for dl in range(2):
        wf[dl] = remote(wt_ref.at[2 * ((y + 2) % 4) + dl], w_pass.at[dl], wf_s.at[dl], wf_r.at[dl],
                        dev(z, xl, core, (y + near[dl]) % 4, xh))
        wf[dl].start()
    for dy in near:
        w_near(dy, 1)
    for dl in range(2):
        own.append(pltpu.make_async_copy(load_ref.at[2 * y + dl], l_all.at[dl, :, pl.ds(0, 128)], loc.at[2 + dl]))
        own[-1].start()
    own.append(pltpu.make_async_copy(spec_ref, spec, loc.at[5]))
    own[-1].start()
    w_arrived(1, 0)
    w_arrived(3, 0)
    for dl in range(2):
        wf[dl].wait_recv()
        wy[2, dl] = remote(w_pass.at[dl], wt_all.at[dl, block_of((y + near[1 - dl]) % 4), :],
                           wy_s.at[1, dl], wy_r.at[1, dl], dev(z, xl, core, (y + near[dl]) % 4, xh))
        wy[2, dl].start()
    for dl in range(2):
        lf[dl] = remote(load_ref.at[2 * ((y + 2) % 4) + dl], l_pass.at[dl], lf_s.at[dl], lf_r.at[dl],
                        dev(z, xl, core, (y + near[dl]) % 4, xh))
        lf[dl].start()
    for dy in near:
        l_near(dy, 0)
    w_arrived(1, 1)
    w_arrived(3, 1)
    w_arrived(2, 0)
    w_arrived(2, 1)
    for c in own:
        c.wait()
    for dl in range(2):
        scale = spec[pl.ds(2 * y + dl, 1), :]
        w = wt_all[dl, lanes256(xh), :]
        wg[dl] = (scale * w.astype(F32)).astype(BF16)
    mate = dev(z, xl, 1 - core, y, xh)
    beside = dev(z, 1 - xl, core, y, xh)
    kept, given = lanes256(xl), lanes256(1 - xl)

    def l_dot(lo, n):
        def product(d):
            return jnp.dot(wt_all[d], l_all[d, :, pl.ds(lo, n)], preferred_element_type=F32)

        return product

    class Group:
        def __init__(self, i, part, send, got, xg, zg, product):
            self.i, self.part, self.send, self.got, self.xg, self.zg = i, part, send, got, xg, zg
            self.product = product
            self.pair = remote(send, got, cc_s.at[i], cc_r.at[i], mate)
            self.side = remote(part.at[given, :], xg, xl_s.at[i], xl_r.at[i], beside)

        def dots(self):
            self.send[...] = self.product(1 - core)
            self.pair.start()
            self.part[...] = self.product(core)

        def over_x(self):
            self.pair.wait_recv()
            self.part[given, :] = self.part[given, :] + self.got[given, :]
            self.side.start()
            self.part[kept, :] = self.part[kept, :] + self.got[kept, :]

        def line(self, k):
            to = (z + k) % 4
            return remote(self.xg.at[part64(to), :], self.zg.at[k - 1],
                          zz_s.at[self.i, k - 1], zz_r.at[self.i, k - 1], dev(to, xl, core, y, xh))

        def over_z(self):
            self.side.wait_recv()
            self.xg[...] = self.xg[...] + self.part[kept, :]
            for k in (1, 3, 2):
                self.line(k).start()

        def total(self):
            for k in (1, 3, 2):
                self.line(k).wait_recv()
            return (self.xg[part64(z), :] + self.zg[0]) + (self.zg[1] + self.zg[2])

        def sent(self):
            self.pair.wait_send()
            self.side.wait_send()
            for k in (1, 3, 2):
                self.line(k).wait_send()

    alike = xl == xh
    differ = xl != xh

    class Specific:
        def __init__(self, i, rows, keep, give):
            self.i, self.rows, self.keep, self.give = i, rows, keep, give
            self.pair = remote(send_s.at[i], got_s.at[i], sc_s.at[i], sc_r.at[i], mate)
            self.side = remote(sum_s.at[i], in_s.at[i], sd_s.at[i], sd_r.at[i], beside)

        def product(self, d):
            return lax.dot_general(wt_all[d, self.rows, :], wg[d], NT, preferred_element_type=F32)

        def dots(self):
            send_s[self.i] = self.product(1 - core)
            self.pair.start()
            part_s[self.i] = self.product(core)

        def line(self, k):
            to = (z + k) % 4
            return remote(part_s.at[self.i, part64(to), :], zg_s.at[self.i, k - 1],
                          sl_s.at[self.i, k - 1], sl_r.at[self.i, k - 1], dev(to, xl, core, y, xh))

        def over_z(self):
            self.pair.wait_recv()
            part_s[self.i] = part_s[self.i] + got_s[self.i]
            for k in (2, 1, 3):
                self.line(k).start()

        def over_x(self):
            for k in (1, 3, 2):
                self.line(k).wait_recv()
            i = self.i
            sum_s[i] = (part_s[i, part64(z), :] + zg_s[i, 0]) + (zg_s[i, 1] + zg_s[i, 2])

            @pl.when(self.give)
            def _():
                self.side.start()

        def total(self):
            self.side.wait_recv()
            return sum_s[self.i] + in_s[self.i]

        def sent(self):
            self.pair.wait_send()
            for k in (1, 3, 2):
                self.line(k).wait_send()

            @pl.when(self.give)
            def _():
                self.side.wait_send()

    g_s = Specific(0, lanes256(xh), alike, differ)
    g_s.dots()
    g_s.over_z()
    for dl in range(2):
        lf[dl].wait_recv()
        ly[2, dl] = remote(l_pass.at[dl], l_all.at[dl, :, pl.ds(128 * SLOT[2], 128)],
                           ly_s.at[1, dl], ly_r.at[1, dl], dev(z, xl, core, (y + near[dl]) % 4, xh))
        ly[2, dl].start()
    for dy in near:
        l_near(dy, 1)
    turn = (z + 2 * core) % 4
    yq = (y + turn) % 4
    yd = (y + 4 - turn) % 4
    f_copy = remote(fcov_ref.at[2 * yd + core], f_rows, f_s, f_r, dev(z, xl, core, yd, xh))
    f_own = pltpu.make_async_copy(fcov_ref.at[day], f_rows, loc.at[4])

    g_s.over_x()
    for dl in range(2):
        for rel in (0, 1, 3, 2):
            wx[rel, dl].wait_recv()
    me_p = 4 * xl + z

    class Straight:
        def __init__(self, i, part, send, got, rs, product):
            self.part, self.send, self.got, self.rs, self.product = part, send, got, rs, product
            self.pair = remote(send, got, cc_s.at[i], cc_r.at[i], mate)

        dots = Group.dots

        def copy(self, k):
            dz, dx = OTHERS[k]
            tz, tx = (z + dz) % 4, (xl + dx) % 2
            return remote(self.part.at[part64(4 * tx + tz), :], self.rs.at[k], rf_s.at[k], rf_r.at[k],
                          dev(tz, tx, core, y, xh))

        def add(self):
            self.pair.wait_recv()
            self.part[...] = self.part[...] + self.got[...]
            for k in range(7):
                self.copy(k).start()

        def total(self):
            for k in range(7):
                self.copy(k).wait_recv()
            total = self.part[part64(me_p), :]
            for k in range(7):
                total = total + self.rs[k]
            return total

        def sent(self):
            self.pair.wait_send()
            for k in range(7):
                self.copy(k).wait_send()

    me8 = 2 * z + xh

    def spread(u, k, block):
        dz, dx = OTHERS[k]
        return remote(red.at[u], e_all.at[part64(z), lanes128(block)], ag_s.at[u, k], ag_r.at[u, k],
                      dev((z + dz) % 4, xl, core, y, (xh + dx) % 2))

    def gather(items):
        blocks = [2 * ((y + rel) % 4) + xh for _, _, rel in items]
        for value, u, _ in items:
            red[u] = value
        for k in range(7):
            for (_, u, _), block in zip(items, blocks):
                spread(u, k, block).start()
        for (value, _, _), block in zip(items, blocks):
            e_all[part64(z), lanes128(block)] = value

    def along(u, k, rel):
        dz, _ = OTHERS[k]
        pair = e_all.at[part64(z), lanes256((y + rel) % 4)]
        return remote(pair, pair, ag_s.at[u, k], ag_r.at[u, k], dev((z + dz) % 4, xl, core, y, xh))

    def gather_x(items):
        for value, u, rel in items:
            block = 2 * ((y + rel) % 4) + xh
            red[u] = value
            spread(u, 6, block).start()
            e_all[part64(z), lanes128(block)] = value

    def gather_z(u, rel):
        spread(u, 6, 0).wait_recv()
        for k in (3, 4, 5):
            along(u, k, rel).start()

    def gathered(u, rel):
        for k in (3, 4, 5):
            along(u, k, rel).wait_recv()

    def gather_sent(u, rel):
        for k in (3, 4, 5):
            along(u, k, rel).wait_send()
        spread(u, 6, 0).wait_send()

    g_o = Group(0, part_o, send_o, got_o, xg_o, zg_o, l_dot(0, 128))
    g_f = Straight(1, part_f, send_f, got_f, rs_f, l_dot(128, 128))
    g_r = Specific(1, lanes256(1 - xh), differ, alike)


    def pair_n(dl, h):
        half = (given, kept)[h]
        return remote(two.at[dl, half, :], got_n.at[half, :], cc_s.at[3 + h], cc_r.at[3 + h], mate)

    def rn(k):
        dz, dx = OTHERS[k]
        tz, tx = (z + dz) % 4, (xl + dx) % 2
        return remote(two.at[core, part64(4 * tx + tz), :], rs_n.at[k], rn_s.at[k], rn_r.at[k],
                      dev(tz, tx, core, y, xh))

    def piece(dl, half, rows):
        return jnp.dot(wt_all[dl, half, rows], l_all[dl, rows, pl.ds(256, 256)], preferred_element_type=F32)

    def near_dot(dl):
        if dl == 0:
            for dy in near:
                ly[dy, 0].wait_recv()
        else:
            for dy in near:
                ly[dy, 2].wait_recv()
        for h, half in enumerate((given, kept)):
            if dl == 0:
                two[dl, half, :] = piece(dl, half, slice(None))
            else:
                two[dl, half, :] = two[dl, half, :] + piece(dl, half, rest)

            @pl.when(core != dl)
            def _():
                pair_n(dl, h).start()

    def near_add(dl):
        @pl.when(core == dl)
        def _():
            for h, half in enumerate((given, kept)):
                pair_n(dl, h).wait_recv()
                two[dl, half, :] = two[dl, half, :] + got_n[half, :]
                for k in range(7):
                    if OTHERS[k][1] == 1 - h:
                        rn(k).start()

    def near_gather(dl, how):
        @pl.when(core == dl)
        def _():
            for k in range(7):
                rn(k).wait_recv()
            total = two[dl, part64(me_p), :]
            for k in range(7):
                total = total + rs_n[k]
            how(((total[:, :128], 2, 1), (total[:, 128:], 3, 3)))

    g_o.dots()
    g_o.over_x()
    near_dot(0)
    g_r.dots()
    g_o.over_z()
    near_add(0)
    g_r.over_z()
    for dl in range(2):
        ly[2, dl].wait_recv()
    g_f.dots()
    gather_x(((g_o.total(), 0, 0),))
    g_f.add()
    near_gather(0, gather_x)
    gather_z(0, 0)
    for c in [*wy.values(), *wx.values(), *wf.values()]:
        c.wait_send()
    for dy in near:
        ly[dy, 1].wait_recv()
    two[1] = piece(1, slice(None), most)

    @pl.when(core == 0)
    def _():
        gather_z(2, 1)
        gather_z(3, 3)

    gather(((g_f.total(), 1, 2),))
    near_dot(1)
    @pl.when(turn == 0)
    def _():
        f_own.start()

    @pl.when(turn != 0)
    def _():
        f_copy.start()

    near_add(1)
    g_r.over_x()
    near_gather(1, gather)

    @pl.when(turn == 0)
    def _():
        f_own.wait()

    @pl.when(turn != 0)
    def _():
        f_copy.wait_recv()

    def left_part(rel):
        at = lanes256((y + rel) % 4)
        return dot_nt(e_all[:, at], f_rows[:, at])

    gathered(0, 0)
    for k in range(7):
        spread(1, k, 0).wait_recv()
    left_val[...] = left_part(0) + left_part(2)
    g_o.sent()
    g_f.sent()

    @pl.when(core == 0)
    def _():
        gathered(2, 1)
        gathered(3, 3)

    @pl.when(core == 1)
    def _():
        for k in range(7):
            spread(2, k, 0).wait_recv()
            spread(3, k, 0).wait_recv()

    left_val[...] += left_part(1) + left_part(3)

    def la(j):
        return remote(left_val.at[part64(j // 2), :], left_buf.at[:, lanes128(2 * yq + xh)],
                      la_s.at[j], la_r.at[me8], dev(j // 2, j % 2, core, y, xl))

    me_t = 2 * z + xl

    def unless(skip, body):
        @pl.when(jnp.logical_not(skip))
        def _():
            body()

    loop(0, 8, lambda j: unless(jnp.logical_and(alike, j == me_t), lambda: la(j).start()))

    @pl.when(alike)
    def _():
        left_buf[:, lanes128(2 * yq + xh)] = left_val[part64(z), :]

    swap = remote(s_red, s_tile, sx_s, sx_r, dev(z, xh, core, y, xl))

    @pl.when(alike)
    def _():
        s_tile[...] = g_s.total()

    @pl.when(differ)
    def _():
        s_red[...] = g_r.total()
        swap.start()

    g_s.sent()
    g_r.sent()
    gather_sent(0, 0)
    for k in range(7):
        spread(1, k, 0).wait_send()

    @pl.when(core == 0)
    def _():
        gather_sent(2, 1)
        gather_sent(3, 3)

    @pl.when(core == 1)
    def _():
        for k in range(7):
            spread(2, k, 0).wait_send()
            spread(3, k, 0).wait_send()

    for k in range(7):
        rn(k).wait_send()

    def la_in(j):
        return remote(left_val.at[part64(0), :], left_buf.at[:, lanes128(0)], la_s.at[0], la_r.at[j], mate)

    loop(0, 8, lambda j: unless(jnp.logical_and(alike, j == me8), lambda: la_in(j).wait_recv()))
    tile = dot_nt(left_buf[...], e_all[...])

    @pl.when(xl != xh)
    def _():
        swap.wait_recv()

    tile = tile + s_tile[...]
    for h in range(2):
        for b in range(4):
            obuf[4 * h + b] = tile[32 * h:32 * h + 32, 64 * b:64 * b + 64]

    def fo(i):
        return remote(obuf.at[i], out_ref.at[day], fo_s.at[i], fo_r.at[day], dev(z, xh, i // 4, i % 4, xl))

    me_o = 4 * core + y
    stay = pltpu.make_async_copy(obuf.at[me_o], out_ref.at[day], loc.at[6])
    loop(0, 8, lambda i: unless(jnp.logical_and(alike, i == me_o), lambda: fo(i).start()))

    @pl.when(alike)
    def _():
        stay.start()

    for c in [*ly.values(), *lf.values()]:
        c.wait_send()
    for h in range(2):
        pair_n(1 - core, h).wait_send()

    @pl.when(xl != xh)
    def _():
        swap.wait_send()

    @pl.when(turn != 0)
    def _():
        f_copy.wait_send()

    loop(0, 8, lambda j: unless(jnp.logical_and(alike, j == me_t), lambda: la(j).wait_send()))

    def fo_in(d):
        return remote(obuf.at[0], out_ref.at[d], fo_s.at[0], fo_r.at[d], mate)

    loop(0, 8, lambda d: unless(jnp.logical_and(alike, d == day), lambda: fo_in(d).wait_recv()))

    @pl.when(alike)
    def _():
        stay.wait()

    loop(0, 8, lambda i: unless(jnp.logical_and(alike, i == me_o), lambda: fo(i).wait_send()))


def shards(loadings, weights, specific, factor_cov):
    assets = loadings.shape[1]
    wt = jnp.swapaxes(weights, 1, 2)
    any_ = pl.BlockSpec(memory_space=pl.ANY)
    dma = pltpu.SemaphoreType.DMA
    return pl.pallas_call(
        kernel,
        out_shape=jax.ShapeDtypeStruct((8, 32, 64), F32),
        in_specs=[any_] * 4,
        out_specs=any_,
        scratch_shapes=[
            pltpu.VMEM((2, 512, assets), BF16),
            pltpu.VMEM((2, assets, 512), BF16),
            pltpu.VMEM((2, 64, assets), BF16),
            pltpu.VMEM((2, assets, 128), BF16),
            pltpu.VMEM((8, assets), F32),
            pltpu.VMEM((2, 256, assets), BF16),
            pltpu.VMEM((128, 1024), F32),
            *[pltpu.VMEM((512, 128), F32)] * 3,
            pltpu.VMEM((256, 128), F32),
            pltpu.VMEM((3, 64, 128), F32),
            *[pltpu.VMEM((512, 128), F32)] * 3,
            pltpu.VMEM((7, 64, 128), F32),
            *[pltpu.VMEM((2, 256, 256), F32)] * 3,
            pltpu.VMEM((2, 3, 64, 256), F32),
            pltpu.VMEM((2, 64, 256), F32),
            pltpu.VMEM((2, 64, 256), F32),
            pltpu.VMEM((2, 512, 256), F32),
            pltpu.VMEM((512, 256), F32),
            pltpu.VMEM((7, 64, 256), F32),
            pltpu.VMEM((4, 64, 128), F32),
            pltpu.VMEM((64, 256), F32),
            pltpu.VMEM((64, 256), F32),
            pltpu.VMEM((256, 1024), F32),
            pltpu.VMEM((256, 128), F32),
            pltpu.VMEM((64, 1024), F32),
            pltpu.VMEM((8, 32, 64), F32),
            dma((3, 2)), dma((3, 2)), dma((3, 3)), dma((3, 3)), dma((4, 2)), dma((4, 2)),
            dma((2,)), dma((2,)), dma((2,)), dma((2,)), dma((7,)), dma, dma,
            dma((5,)), dma((5,)), dma((3,)), dma((3,)), dma((3, 3)), dma((3, 3)), dma((7,)), dma((7,)), dma((7,)), dma((7,)),
            dma((4, 7)), dma((4, 7)), dma, dma,
            dma((2,)), dma((2,)), dma((2, 3)), dma((2, 3)), dma((2,)), dma((2,)), dma((8,)), dma((8,)), dma((8,)), dma((8,)),
        ],
        compiler_params=pltpu.CompilerParams(collective_id=0, has_side_effects=True),
    )(loadings, wt, specific, factor_cov)


def solution(mesh):
    in_specs = (P(None, "row", "col"), P(None, "row", "col"), P(None, "row"), P(None, "col", None))
    out_specs = P(None, "row", "col")
    return jax.shard_map(shards, mesh=mesh, in_specs=in_specs, out_specs=out_specs, check_vma=False)
```

```python
import jax
import jax.numpy as jnp
from jax import lax
from jax.experimental import pallas as pl
from jax.experimental.pallas import tpu as pltpu
from jax.sharding import PartitionSpec as P

MESH = pl.DeviceIdType.MESH
F32 = jnp.float32
BF16 = jnp.bfloat16
NT = (((1,), (1,)), ((), ()))
SLOT = {0: 0, 2: 1, 1: 2, 3: 3}
OTHERS = ((2, 1), (1, 1), (3, 1), (2, 0), (1, 0), (3, 0), (0, 1))


def halves(value):
    top = value.astype(BF16)
    return top, (value - top.astype(F32)).astype(BF16)


def dot_nt(a, b):
    (a_top, a_low), (b_top, b_low) = halves(a), halves(b)

    def one(p, q):
        return lax.dot_general(p, q, NT, preferred_element_type=F32)

    return one(a_top, b_top) + (one(a_top, b_low) + one(a_low, b_top))


def kernel(load_ref, wt_ref, spec_ref, fcov_ref, out_ref,
           wt_all, l_all, w_pass, l_pass, spec, wg, f_rows,
           part_o, send_o, got_o, xg_o, zg_o, part_f, send_f, got_f, rs_f,
           part_s, send_s, got_s, zg_s, sum_s, in_s,
           two, got_n, rs_n, red, s_red, s_tile, e_all, left_val, left_buf, obuf,
           wy_s, wy_r, ly_s, ly_r, wx_s, wx_r, wf_s, wf_r, lf_s, lf_r, loc, f_s, f_r,
           cc_s, cc_r, xl_s, xl_r, zz_s, zz_r, rf_s, rf_r, rn_s, rn_r, ag_s, ag_r, sx_s, sx_r, sd_s, sd_r, sl_s, sl_r, sc_s, sc_r,
           la_s, la_r, fo_s, fo_r):
    row, col = lax.axis_index("row"), lax.axis_index("col")
    z, xl, core = row // 4, (row // 2) % 2, row % 2
    y, xh = col // 2, col % 2
    day = 2 * y + core

    def dev(z_, xl_, core_, y_, xh_):
        return (z_ * 4 + xl_ * 2 + core_, y_ * 2 + xh_)

    def remote(src, dst, ssem, rsem, to):
        return pltpu.make_async_remote_copy(
            src_ref=src, dst_ref=dst, send_sem=ssem, recv_sem=rsem,
            device_id=to, device_id_type=MESH)

    def loop(lo, hi, body):
        def step(k, _):
            body(k)
            return 0

        lax.fori_loop(lo, hi, step, 0)

    def part64(i):
        return pl.ds(pl.multiple_of(i * 64, 64), 64)

    def lanes128(i):
        return pl.ds(pl.multiple_of(i * 128, 128), 128)

    def lanes256(i):
        return pl.ds(pl.multiple_of(i * 256, 256), 256)

    bar = pltpu.get_barrier_semaphore()

    def greet(to):
        pl.semaphore_signal(bar, inc=1, device_id=to, device_id_type=MESH)

    for k in (1, 2, 3):
        greet(dev((z + k) % 4, xl, core, y, xh))
    for k in (1, 3):
        greet(dev(z, xl, core, (y + k) % 4, xh))
    greet(dev(z, 1 - xl, core, y, xh))
    greet(dev(z, xl, core, y, 1 - xh))
    greet(dev(z, xl, 1 - core, y, xh))
    pl.semaphore_wait(bar, 8)

    def block_of(b):
        return part64(4 * xh + b)

    here = block_of(y)
    across = dev(z, xl, core, y, 1 - xh)
    near = (1, 3)
    assets = l_all.shape[1]
    most, rest = pl.ds(0, 3 * assets // 4), pl.ds(3 * assets // 4, assets // 4)
    own = []
    wy, wx, ly, wf, lf = {}, {}, {}, {}, {}

    def w_near(dy, dl):
        ty = (y + dy) % 4
        wy[dy, dl] = remote(wt_ref.at[2 * ty + dl], wt_all.at[dl, here, :],
                            wy_s.at[dy - 1, dl], wy_r.at[dy - 1, dl], dev(z, xl, core, ty, xh))
        wy[dy, dl].start()

    def w_across(rel, dl):
        rows = block_of((y + rel) % 4)
        src = wt_ref.at[2 * y + dl] if rel == 0 else wt_all.at[dl, rows, :]
        wx[rel, dl] = remote(src, wt_all.at[dl, rows, :], wx_s.at[rel, dl], wx_r.at[rel, dl], across)
        wx[rel, dl].start()

    def w_arrived(rel, dl):
        wy[4 - rel, dl].wait_recv()
        w_across(rel, dl)

    def l_near(dy, dl):
        ty = (y + dy) % 4
        slot = pl.ds(128 * SLOT[4 - dy], 128)
        to = dev(z, xl, core, ty, xh)
        if dl == 0:
            ly[dy, dl] = remote(load_ref.at[2 * ty], l_all.at[0, :, slot],
                                ly_s.at[dy - 1, 0], ly_r.at[dy - 1, 0], to)
            ly[dy, dl].start()
            return
        for rows, i in ((most, 1), (rest, 2)):
            ly[dy, i] = remote(load_ref.at[2 * ty + 1, rows, :], l_all.at[1, rows, slot],
                               ly_s.at[dy - 1, i], ly_r.at[dy - 1, i], to)
            ly[dy, i].start()

    for dy in near:
        w_near(dy, 0)
    for dl in range(2):
        w_across(0, dl)
        own.append(pltpu.make_async_copy(wt_ref.at[2 * y + dl], wt_all.at[dl, here, :], loc.at[dl]))
        own[-1].start()
    for dl in range(2):
        wf[dl] = remote(wt_ref.at[2 * ((y + 2) % 4) + dl], w_pass.at[dl], wf_s.at[dl], wf_r.at[dl],
                        dev(z, xl, core, (y + near[dl]) % 4, xh))
        wf[dl].start()
    for dy in near:
        w_near(dy, 1)
    for dl in range(2):
        own.append(pltpu.make_async_copy(load_ref.at[2 * y + dl], l_all.at[dl, :, pl.ds(0, 128)], loc.at[2 + dl]))
        own[-1].start()
    own.append(pltpu.make_async_copy(spec_ref, spec, loc.at[5]))
    own[-1].start()
    w_arrived(1, 0)
    w_arrived(3, 0)
    for dl in range(2):
        wf[dl].wait_recv()
        wy[2, dl] = remote(w_pass.at[dl], wt_all.at[dl, block_of((y + near[1 - dl]) % 4), :],
                           wy_s.at[1, dl], wy_r.at[1, dl], dev(z, xl, core, (y + near[dl]) % 4, xh))
        wy[2, dl].start()
    for dl in range(2):
        lf[dl] = remote(load_ref.at[2 * ((y + 2) % 4) + dl], l_pass.at[dl], lf_s.at[dl], lf_r.at[dl],
                        dev(z, xl, core, (y + near[dl]) % 4, xh))
        lf[dl].start()
    for dy in near:
        l_near(dy, 0)
    w_arrived(1, 1)
    w_arrived(3, 1)
    w_arrived(2, 0)
    w_arrived(2, 1)
    for c in own:
        c.wait()
    for dl in range(2):
        scale = spec[pl.ds(2 * y + dl, 1), :]
        w = wt_all[dl, lanes256(xh), :]
        wg[dl] = (scale * w.astype(F32)).astype(BF16)
    mate = dev(z, xl, 1 - core, y, xh)
    beside = dev(z, 1 - xl, core, y, xh)
    kept, given = lanes256(xl), lanes256(1 - xl)

    def l_dot(lo, n):
        def product(d):
            return jnp.dot(wt_all[d], l_all[d, :, pl.ds(lo, n)], preferred_element_type=F32)

        return product

    class Group:
        def __init__(self, i, part, send, got, xg, zg, product):
            self.i, self.part, self.send, self.got, self.xg, self.zg = i, part, send, got, xg, zg
            self.product = product
            self.pair = remote(send, got, cc_s.at[i], cc_r.at[i], mate)
            self.side = remote(part.at[given, :], xg, xl_s.at[i], xl_r.at[i], beside)

        def dots(self):
            self.send[...] = self.product(1 - core)
            self.pair.start()
            self.part[...] = self.product(core)

        def over_x(self):
            self.pair.wait_recv()
            self.part[given, :] = self.part[given, :] + self.got[given, :]
            self.side.start()
            self.part[kept, :] = self.part[kept, :] + self.got[kept, :]

        def line(self, k):
            to = (z + k) % 4
            return remote(self.xg.at[part64(to), :], self.zg.at[k - 1],
                          zz_s.at[self.i, k - 1], zz_r.at[self.i, k - 1], dev(to, xl, core, y, xh))

        def over_z(self):
            self.side.wait_recv()
            self.xg[...] = self.xg[...] + self.part[kept, :]
            for k in (1, 3, 2):
                self.line(k).start()

        def total(self):
            for k in (1, 3, 2):
                self.line(k).wait_recv()
            return (self.xg[part64(z), :] + self.zg[0]) + (self.zg[1] + self.zg[2])

        def sent(self):
            self.pair.wait_send()
            self.side.wait_send()
            for k in (1, 3, 2):
                self.line(k).wait_send()

    alike = xl == xh
    differ = xl != xh

    class Specific:
        def __init__(self, i, rows, keep, give):
            self.i, self.rows, self.keep, self.give = i, rows, keep, give
            self.pair = remote(send_s.at[i], got_s.at[i], sc_s.at[i], sc_r.at[i], mate)
            self.side = remote(sum_s.at[i], in_s.at[i], sd_s.at[i], sd_r.at[i], beside)

        def product(self, d):
            return lax.dot_general(wt_all[d, self.rows, :], wg[d], NT, preferred_element_type=F32)

        def dots(self):
            send_s[self.i] = self.product(1 - core)
            self.pair.start()
            part_s[self.i] = self.product(core)

        def line(self, k):
            to = (z + k) % 4
            return remote(part_s.at[self.i, part64(to), :], zg_s.at[self.i, k - 1],
                          sl_s.at[self.i, k - 1], sl_r.at[self.i, k - 1], dev(to, xl, core, y, xh))

        def over_z(self):
            self.pair.wait_recv()
            part_s[self.i] = part_s[self.i] + got_s[self.i]
            for k in (2, 1, 3):
                self.line(k).start()

        def over_x(self):
            for k in (1, 3, 2):
                self.line(k).wait_recv()
            i = self.i
            sum_s[i] = (part_s[i, part64(z), :] + zg_s[i, 0]) + (zg_s[i, 1] + zg_s[i, 2])

            @pl.when(self.give)
            def _():
                self.side.start()

        def total(self):
            self.side.wait_recv()
            return sum_s[self.i] + in_s[self.i]

        def sent(self):
            self.pair.wait_send()
            for k in (1, 3, 2):
                self.line(k).wait_send()

            @pl.when(self.give)
            def _():
                self.side.wait_send()

    g_s = Specific(0, lanes256(xh), alike, differ)
    g_s.dots()
    g_s.over_z()
    for dl in range(2):
        lf[dl].wait_recv()
        ly[2, dl] = remote(l_pass.at[dl], l_all.at[dl, :, pl.ds(128 * SLOT[2], 128)],
                           ly_s.at[1, dl], ly_r.at[1, dl], dev(z, xl, core, (y + near[dl]) % 4, xh))
        ly[2, dl].start()
    for dy in near:
        l_near(dy, 1)
    turn = (z + 2 * core) % 4
    yq = (y + turn) % 4
    yd = (y + 4 - turn) % 4
    f_copy = remote(fcov_ref.at[2 * yd + core], f_rows, f_s, f_r, dev(z, xl, core, yd, xh))
    f_own = pltpu.make_async_copy(fcov_ref.at[day], f_rows, loc.at[4])

    g_s.over_x()
    for dl in range(2):
        for rel in (0, 1, 3, 2):
            wx[rel, dl].wait_recv()
    me_p = 4 * xl + z

    class Straight:
        def __init__(self, i, part, send, got, rs, product):
            self.part, self.send, self.got, self.rs, self.product = part, send, got, rs, product
            self.pair = remote(send, got, cc_s.at[i], cc_r.at[i], mate)

        dots = Group.dots

        def copy(self, k):
            dz, dx = OTHERS[k]
            tz, tx = (z + dz) % 4, (xl + dx) % 2
            return remote(self.part.at[part64(4 * tx + tz), :], self.rs.at[k], rf_s.at[k], rf_r.at[k],
                          dev(tz, tx, core, y, xh))

        def add(self):
            self.pair.wait_recv()
            self.part[...] = self.part[...] + self.got[...]
            for k in range(7):
                self.copy(k).start()

        def total(self):
            for k in range(7):
                self.copy(k).wait_recv()
            total = self.part[part64(me_p), :]
            for k in range(7):
                total = total + self.rs[k]
            return total

        def sent(self):
            self.pair.wait_send()
            for k in range(7):
                self.copy(k).wait_send()

    me8 = 2 * z + xh

    def spread(u, k, block):
        dz, dx = OTHERS[k]
        return remote(red.at[u], e_all.at[part64(z), lanes128(block)], ag_s.at[u, k], ag_r.at[u, k],
                      dev((z + dz) % 4, xl, core, y, (xh + dx) % 2))

    def gather(items):
        blocks = [2 * ((y + rel) % 4) + xh for _, _, rel in items]
        for value, u, _ in items:
            red[u] = value
        for k in range(7):
            for (_, u, _), block in zip(items, blocks):
                spread(u, k, block).start()
        for (value, _, _), block in zip(items, blocks):
            e_all[part64(z), lanes128(block)] = value

    def along(u, k, rel):
        dz, _ = OTHERS[k]
        pair = e_all.at[part64(z), lanes256((y + rel) % 4)]
        return remote(pair, pair, ag_s.at[u, k], ag_r.at[u, k], dev((z + dz) % 4, xl, core, y, xh))

    def gather_x(items):
        for value, u, rel in items:
            block = 2 * ((y + rel) % 4) + xh
            red[u] = value
            spread(u, 6, block).start()
            e_all[part64(z), lanes128(block)] = value

    def gather_z(u, rel):
        spread(u, 6, 0).wait_recv()
        for k in (3, 4, 5):
            along(u, k, rel).start()

    def gathered(u, rel):
        for k in (3, 4, 5):
            along(u, k, rel).wait_recv()

    def gather_sent(u, rel):
        for k in (3, 4, 5):
            along(u, k, rel).wait_send()
        spread(u, 6, 0).wait_send()

    g_o = Group(0, part_o, send_o, got_o, xg_o, zg_o, l_dot(0, 128))
    g_f = Straight(1, part_f, send_f, got_f, rs_f, l_dot(128, 128))
    g_r = Specific(1, lanes256(1 - xh), differ, alike)


    def pair_n(dl, h):
        half = (given, kept)[h]
        return remote(two.at[dl, half, :], got_n.at[half, :], cc_s.at[3 + h], cc_r.at[3 + h], mate)

    def rn(k):
        dz, dx = OTHERS[k]
        tz, tx = (z + dz) % 4, (xl + dx) % 2
        return remote(two.at[core, part64(4 * tx + tz), :], rs_n.at[k], rn_s.at[k], rn_r.at[k],
                      dev(tz, tx, core, y, xh))

    def piece(dl, half, rows):
        return jnp.dot(wt_all[dl, half, rows], l_all[dl, rows, pl.ds(256, 256)], preferred_element_type=F32)

    def near_dot(dl):
        if dl == 0:
            for dy in near:
                ly[dy, 0].wait_recv()
        else:
            for dy in near:
                ly[dy, 2].wait_recv()
        for h, half in enumerate((given, kept)):
            if dl == 0:
                two[dl, half, :] = piece(dl, half, slice(None))
            else:
                two[dl, half, :] = two[dl, half, :] + piece(dl, half, rest)

            @pl.when(core != dl)
            def _():
                pair_n(dl, h).start()

    def near_add(dl):
        @pl.when(core == dl)
        def _():
            for h, half in enumerate((given, kept)):
                pair_n(dl, h).wait_recv()
                two[dl, half, :] = two[dl, half, :] + got_n[half, :]
                for k in range(7):
                    if OTHERS[k][1] == 1 - h:
                        rn(k).start()

    def near_gather(dl, how):
        @pl.when(core == dl)
        def _():
            for k in range(7):
                rn(k).wait_recv()
            total = two[dl, part64(me_p), :]
            for k in range(7):
                total = total + rs_n[k]
            how(((total[:, :128], 2, 1), (total[:, 128:], 3, 3)))

    g_o.dots()
    g_o.over_x()
    near_dot(0)
    g_r.dots()
    g_o.over_z()
    near_add(0)
    g_r.over_z()
    for dl in range(2):
        ly[2, dl].wait_recv()
    g_f.dots()
    gather_x(((g_o.total(), 0, 0),))
    g_f.add()
    near_gather(0, gather_x)
    gather_z(0, 0)
    for c in [*wy.values(), *wx.values(), *wf.values()]:
        c.wait_send()
    for dy in near:
        ly[dy, 1].wait_recv()
    two[1] = piece(1, slice(None), most)

    @pl.when(core == 0)
    def _():
        gather_z(2, 1)
        gather_z(3, 3)

    gather(((g_f.total(), 1, 2),))
    near_dot(1)
    @pl.when(turn == 0)
    def _():
        f_own.start()

    @pl.when(turn != 0)
    def _():
        f_copy.start()

    near_add(1)
    g_r.over_x()
    near_gather(1, gather)

    @pl.when(turn == 0)
    def _():
        f_own.wait()

    @pl.when(turn != 0)
    def _():
        f_copy.wait_recv()

    def left_part(rel):
        at = lanes256((y + rel) % 4)
        return dot_nt(e_all[:, at], f_rows[:, at])

    gathered(0, 0)
    for k in range(7):
        spread(1, k, 0).wait_recv()
    left_val[...] = left_part(0) + left_part(2)
    g_o.sent()
    g_f.sent()

    @pl.when(core == 0)
    def _():
        gathered(2, 1)
        gathered(3, 3)

    @pl.when(core == 1)
    def _():
        for k in range(7):
            spread(2, k, 0).wait_recv()
            spread(3, k, 0).wait_recv()

    left_val[...] += left_part(1) + left_part(3)

    def la(j):
        return remote(left_val.at[part64(j // 2), :], left_buf.at[:, lanes128(2 * yq + xh)],
                      la_s.at[j], la_r.at[me8], dev(j // 2, j % 2, core, y, xl))

    me_t = 2 * z + xl

    def unless(skip, body):
        @pl.when(jnp.logical_not(skip))
        def _():
            body()

    loop(0, 8, lambda j: unless(jnp.logical_and(alike, j == me_t), lambda: la(j).start()))

    @pl.when(alike)
    def _():
        left_buf[:, lanes128(2 * yq + xh)] = left_val[part64(z), :]

    swap = remote(s_red, s_tile, sx_s, sx_r, dev(z, xh, core, y, xl))

    @pl.when(alike)
    def _():
        s_tile[...] = g_s.total()

    @pl.when(differ)
    def _():
        s_red[...] = g_r.total()
        swap.start()

    g_s.sent()
    g_r.sent()
    gather_sent(0, 0)
    for k in range(7):
        spread(1, k, 0).wait_send()

    @pl.when(core == 0)
    def _():
        gather_sent(2, 1)
        gather_sent(3, 3)

    @pl.when(core == 1)
    def _():
        for k in range(7):
            spread(2, k, 0).wait_send()
            spread(3, k, 0).wait_send()

    for k in range(7):
        rn(k).wait_send()

    def la_in(j):
        return remote(left_val.at[part64(0), :], left_buf.at[:, lanes128(0)], la_s.at[0], la_r.at[j], mate)

    loop(0, 8, lambda j: unless(jnp.logical_and(alike, j == me8), lambda: la_in(j).wait_recv()))

    @pl.when(differ)
    def _():
        swap.wait_recv()

    def fo(i):
        return remote(obuf.at[i], out_ref.at[day], fo_s.at[i], fo_r.at[day], dev(z, xh, i // 4, i % 4, xl))

    me_o = 4 * core + y
    stay = pltpu.make_async_copy(obuf.at[me_o], out_ref.at[day], loc.at[6])
    for c in range(2):
        cols = slice(128 * c, 128 * c + 128)
        tile = dot_nt(left_buf[...], e_all[cols, :]) + s_tile[:, cols]
        for h in range(2):
            for b in range(2):
                i = 4 * h + 2 * c + b
                obuf[i] = tile[32 * h:32 * h + 32, 64 * b:64 * b + 64]
                unless(jnp.logical_and(alike, i == me_o), lambda: fo(i).start())

    @pl.when(alike)
    def _():
        stay.start()

    for c in [*ly.values(), *lf.values()]:
        c.wait_send()
    for h in range(2):
        pair_n(1 - core, h).wait_send()

    @pl.when(xl != xh)
    def _():
        swap.wait_send()

    @pl.when(turn != 0)
    def _():
        f_copy.wait_send()

    loop(0, 8, lambda j: unless(jnp.logical_and(alike, j == me_t), lambda: la(j).wait_send()))

    def fo_in(d):
        return remote(obuf.at[0], out_ref.at[d], fo_s.at[0], fo_r.at[d], mate)

    loop(0, 8, lambda d: unless(jnp.logical_and(alike, d == day), lambda: fo_in(d).wait_recv()))

    @pl.when(alike)
    def _():
        stay.wait()

    loop(0, 8, lambda i: unless(jnp.logical_and(alike, i == me_o), lambda: fo(i).wait_send()))


def shards(loadings, weights, specific, factor_cov):
    assets = loadings.shape[1]
    wt = jnp.swapaxes(weights, 1, 2)
    any_ = pl.BlockSpec(memory_space=pl.ANY)
    dma = pltpu.SemaphoreType.DMA
    return pl.pallas_call(
        kernel,
        out_shape=jax.ShapeDtypeStruct((8, 32, 64), F32),
        in_specs=[any_] * 4,
        out_specs=any_,
        scratch_shapes=[
            pltpu.VMEM((2, 512, assets), BF16),
            pltpu.VMEM((2, assets, 512), BF16),
            pltpu.VMEM((2, 64, assets), BF16),
            pltpu.VMEM((2, assets, 128), BF16),
            pltpu.VMEM((8, assets), F32),
            pltpu.VMEM((2, 256, assets), BF16),
            pltpu.VMEM((128, 1024), F32),
            *[pltpu.VMEM((512, 128), F32)] * 3,
            pltpu.VMEM((256, 128), F32),
            pltpu.VMEM((3, 64, 128), F32),
            *[pltpu.VMEM((512, 128), F32)] * 3,
            pltpu.VMEM((7, 64, 128), F32),
            *[pltpu.VMEM((2, 256, 256), F32)] * 3,
            pltpu.VMEM((2, 3, 64, 256), F32),
            pltpu.VMEM((2, 64, 256), F32),
            pltpu.VMEM((2, 64, 256), F32),
            pltpu.VMEM((2, 512, 256), F32),
            pltpu.VMEM((512, 256), F32),
            pltpu.VMEM((7, 64, 256), F32),
            pltpu.VMEM((4, 64, 128), F32),
            pltpu.VMEM((64, 256), F32),
            pltpu.VMEM((64, 256), F32),
            pltpu.VMEM((256, 1024), F32),
            pltpu.VMEM((256, 128), F32),
            pltpu.VMEM((64, 1024), F32),
            pltpu.VMEM((8, 32, 64), F32),
            dma((3, 2)), dma((3, 2)), dma((3, 3)), dma((3, 3)), dma((4, 2)), dma((4, 2)),
            dma((2,)), dma((2,)), dma((2,)), dma((2,)), dma((7,)), dma, dma,
            dma((5,)), dma((5,)), dma((3,)), dma((3,)), dma((3, 3)), dma((3, 3)), dma((7,)), dma((7,)), dma((7,)), dma((7,)),
            dma((4, 7)), dma((4, 7)), dma, dma,
            dma((2,)), dma((2,)), dma((2, 3)), dma((2, 3)), dma((2,)), dma((2,)), dma((8,)), dma((8,)), dma((8,)), dma((8,)),
        ],
        compiler_params=pltpu.CompilerParams(collective_id=0, has_side_effects=True),
    )(loadings, wt, specific, factor_cov)


def solution(mesh):
    in_specs = (P(None, "row", "col"), P(None, "row", "col"), P(None, "row"), P(None, "col", None))
    out_specs = P(None, "row", "col")
    return jax.shard_map(shards, mesh=mesh, in_specs=in_specs, out_specs=out_specs, check_vma=False)
```
